32 devices in a mesh: seq: 2 (over y), fsdp: 4 (over z), rep: 4 (over x, core).
Axes of the slice: x: 2, y: 2, z: 4, core: 2. Of those that a mesh axis runs over, the one named last changes fastest.
Arguments:
- hidden_in: bfloat16 [16, 512, 1024], P(('fsdp', 'rep'), 'seq'), may hold values from -6 to 6
- encoder_states: bfloat16 [16, 1536, 1024], P(('fsdp', 'rep'), 'seq'), may hold values from -6 to 6
- seq_lengths: int32 [16, 4], P(('fsdp', 'rep')), may hold values from 1 to 320, 512 in all within a row
- deal: int32 [16, 512], P(('fsdp', 'rep')), may hold values from 0 to 511, each once within a row
- gain_self: bfloat16 [1024], P('fsdp'), may hold values from 0.5 to 1.5
- w_self_in: bfloat16 [1024, 3072], P('fsdp'), may hold values from -0.1875 to 0.1875
- w_self_out: bfloat16 [1024, 1024], P('fsdp'), may hold values from -3 to 3
- rel_table: bfloat16 [512], P('fsdp'), may hold values from -6 to 6
- gain_cross: bfloat16 [1024], P('fsdp'), may hold values from 0.5 to 1.5
- w_cross_q: bfloat16 [1024, 1024], P('fsdp'), may hold values from -0.1875 to 0.1875
- w_cross_kv: bfloat16 [1024, 2048], P('fsdp'), may hold values from -0.1875 to 0.1875
- w_cross_out: bfloat16 [1024, 1024], P('fsdp'), may hold values from -3 to 3
- gain_ffn: bfloat16 [1024], P('fsdp'), may hold values from 0.5 to 1.5
- w_gate_up: bfloat16 [1024, 5632], P('fsdp'), may hold values from -0.1875 to 0.1875
- w_down: bfloat16 [2816, 1024], P('fsdp'), may hold values from -0.109375 to 0.109375
- grad_out: bfloat16 [16, 512, 1024], P(('fsdp', 'rep'), 'seq'), may hold values from -6 to 6
Outputs:
- block_out: bfloat16 [16, 512, 1024], P(('fsdp', 'rep'), 'seq')
- input_grad: bfloat16 [16, 512, 1024], P(('fsdp', 'rep'), 'seq')
- encoder_grad: bfloat16 [16, 1536, 1024], P(('fsdp', 'rep'), 'seq')
- grad_gain_self: float32 [1024], P(('seq', 'fsdp'))
- grad_w_self_in: float32 [1024, 3072], P(('seq', 'fsdp'))
- grad_w_self_out: float32 [1024, 1024], P(('seq', 'fsdp'))
- grad_rel_table: float32 [512], P(('seq', 'fsdp'))
- grad_gain_cross: float32 [1024], P(('seq', 'fsdp'))
- grad_w_cross_q: float32 [1024, 1024], P(('seq', 'fsdp'))
- grad_w_cross_kv: float32 [1024, 2048], P(('seq', 'fsdp'))
- grad_w_cross_out: float32 [1024, 1024], P(('seq', 'fsdp'))
- grad_gain_ffn: float32 [1024], P(('seq', 'fsdp'))
- grad_w_gate_up: float32 [1024, 5632], P(('seq', 'fsdp'))
- grad_w_down: float32 [2816, 1024], P(('seq', 'fsdp'))
The draws below stay inside these ranges and needn't reach their ends.
Inputs may be any that keep to these rules, and one draw needn't show every extreme that they name: Each row of a group is a permutation; dealt row r of group g holds the token of given position deal[g, r]. `seq_lengths`: the 4 lengths of a group sum to 512, the largest is 320; the sequences lie end to end in the given order, and sequence s owns encoder rows s * 384 to (s + 1) * 384 - 1.
All inputs are finite; a program needn't handle non-finite values.
Results may differ from the reference program's by a relative error of at most 0.02.
Values may be sent and summed in bfloat16 or wider, within the bound.
A program may use at most 256 MiB of HBM per device.

```python
import math
import jax
import jax.numpy as jnp
import numpy as np
from jax import lax

D = 1024
HEADS = 16
HD = 64
FF = 2816
BUCKETS = 32
ENC = 384
NSEQ_G = 4
GROUPS = 16
GTOK = 512
ENC_G = 1536
BLK = 512
MAXLEN = 320


def steps_of(own_key, dims, pieces, least, high):
    level = 1.0
    for axis_at, blocks in pieces:
        draws = jax.random.uniform(jax.random.fold_in(jax.random.fold_in(own_key, 6), axis_at), (blocks,), jnp.float32, least / len(pieces), high / len(pieces))
        level = level * jnp.repeat(jnp.exp(draws), dims[axis_at] // blocks).reshape((-1,) + (1,) * (len(dims) - 1 - axis_at))
    return level


def split_up(number_of, total, limit, lean):
    loads = [(1 << 20) // math.isqrt(grade ** lean) + 1 for grade in range(2, number_of + 1)]
    rest, holding = total - limit - (number_of - 1), [1] * (number_of - 1)
    while rest > 0:
        movable = [i for i in range(number_of - 1) if holding[i] < limit]
        mass, budget = sum([loads[i] for i in movable]), rest
        for i in movable:
            addition = min(limit - holding[i], max(1, budget * loads[i] // mass), rest)
            holding[i] = holding[i] + addition
            rest = rest - addition
    return np.array([limit] + holding)


def ragged_sizes(rng, number_of, total, limit, lean):
    if number_of == 2:
        one = jax.random.randint(rng, (), max(1, total - limit), min(limit, total - 1) + 1)
        return jnp.stack([one, total - one])
    tallies = jnp.asarray(split_up(number_of, total, limit, lean), jnp.int32)
    pairs = (number_of - 1) // 2
    source_of, sink = tallies[1:1 + 2 * pairs:2], tallies[2:2 + 2 * pairs:2]
    margin = jnp.minimum(source_of - 1, limit - sink)
    moved = jax.random.randint(jax.random.fold_in(rng, 1), (pairs,), 0, 1 << 20) % (margin + 1)
    tallies = tallies.at[1:1 + 2 * pairs:2].set(source_of - moved).at[2:2 + 2 * pairs:2].set(sink + moved)
    return tallies[jax.random.permutation(jax.random.fold_in(rng, 2), number_of)]


def noise(own_key, extent, deviation, bound, cuts=(), kind=jnp.bfloat16):
    result = jax.random.normal(own_key, extent, jnp.float32) * deviation
    if len(cuts) > 0:
        result = steps_of(own_key, extent, cuts, -0.22, 0.18) * result
    return jnp.clip(result, min=-bound, max=bound).astype(kind)


def setup_inputs(seed: int = 0) -> dict:
    arg_keys = jax.random.split(jax.random.key(seed), 17)
    hidden_in = noise(arg_keys[0], (GROUPS, GTOK, D), 1.0, 6.0, ((0, 16), (1, 2)))
    encoder_states = noise(arg_keys[1], (GROUPS, ENC_G, D), 1.0, 6.0, ((0, 16), (1, 2)))
    seq_lengths = jax.vmap(lambda own: ragged_sizes(own, NSEQ_G, GTOK, MAXLEN, 2))(jax.random.split(arg_keys[2], GROUPS)).reshape((GROUPS, NSEQ_G)).astype(jnp.int32)
    deal = jax.vmap(lambda own: jax.random.permutation(own, GTOK))(jax.random.split(arg_keys[3], GROUPS)).reshape((GROUPS, GTOK)).astype(jnp.int32)
    gain_self = jnp.clip(1.0 + 0.1 * jax.random.normal(arg_keys[4], (D,), jnp.float32), 0.5, 1.5).astype(jnp.bfloat16)
    w_self_in = noise(arg_keys[5], (D, 3 * D), D ** -0.5, 0.1875, ((0, 4),))
    w_self_out = noise(arg_keys[6], (D, D), (D // 256) ** -0.5, 3.0, ((0, 4),))
    rel_table = noise(arg_keys[7], (HEADS * BUCKETS,), 1.5, 6.0, ((0, 4),))
    gain_cross = jnp.clip(1.0 + 0.1 * jax.random.normal(arg_keys[8], (D,), jnp.float32), 0.5, 1.5).astype(jnp.bfloat16)
    w_cross_q = noise(arg_keys[9], (D, D), D ** -0.5, 0.1875, ((0, 4),))
    w_cross_kv = noise(arg_keys[10], (D, 2 * D), D ** -0.5, 0.1875, ((0, 4),))
    w_cross_out = noise(arg_keys[11], (D, D), (D // 256) ** -0.5, 3.0, ((0, 4),))
    gain_ffn = jnp.clip(1.0 + 0.1 * jax.random.normal(arg_keys[12], (D,), jnp.float32), 0.5, 1.5).astype(jnp.bfloat16)
    w_gate_up = noise(arg_keys[13], (D, 2 * FF), D ** -0.5, 0.1875, ((0, 4),))
    w_down = noise(arg_keys[14], (FF, D), FF ** -0.5, 0.109375, ((0, 4),))
    grad_out = noise(arg_keys[15], (GROUPS, GTOK, D), 1.0, 6.0, ((0, 16), (1, 2)))
    return {"hidden_in": hidden_in, "encoder_states": encoder_states, "seq_lengths": seq_lengths, "deal": deal, "gain_self": gain_self, "w_self_in": w_self_in, "w_self_out": w_self_out, "rel_table": rel_table, "gain_cross": gain_cross, "w_cross_q": w_cross_q, "w_cross_kv": w_cross_kv, "w_cross_out": w_cross_out, "gain_ffn": gain_ffn, "w_gate_up": w_gate_up, "w_down": w_down, "grad_out": grad_out}


@jax.custom_vjp
def low(v):
    return lax.optimization_barrier(v.astype(jnp.bfloat16)).astype(jnp.float32)

@jax.custom_vjp
def low_back(v):
    return v

def low_keep(v):
    return (low(v), None)

def low_pass(kept, grad):
    return (grad,)

def back_keep(v):
    return (v, None)

def back_low(kept, grad):
    return (low(grad),)
low.defvjp(low_keep, low_pass)
low_back.defvjp(back_keep, back_low)
norm_eps = 1e-06
score_factor = 0.125
masked_score = -1e+30
bucket_edges = [int(edge_value) for edge_value in np.ceil(16.0 * 8.0 ** (np.arange(1, 16) / 16.0))]

def bucket_of(distance):
    far_count = jnp.zeros_like(distance)
    for edge_value in bucket_edges:
        far_count = far_count + (distance >= edge_value).astype(jnp.int32)
    return jnp.where(distance < 16, distance, 16 + far_count)

def rms_scale(values, gain):
    return values * lax.rsqrt(lax.optimization_barrier(jnp.mean(values * values, axis=-1, keepdims=True)) + norm_eps) * gain

def matmul(left, right):
    return jnp.dot(left, right, precision=lax.Precision.HIGHEST)

def segment_ids(lengths, count):
    seq_ends = jnp.cumsum(lengths)
    places = jnp.arange(count, dtype=jnp.int32)
    return lax.optimization_barrier(jnp.sum((places[:, None] >= seq_ends[None, :]).astype(jnp.int32), axis=1))

def split_heads(values):
    return values.reshape(values.shape[0], HEADS, HD).transpose(1, 0, 2)

def join_blocks(blocks):
    stacked = blocks.transpose(1, 0, 2, 3).reshape(HEADS, GTOK, HD)
    return stacked.transpose(1, 0, 2).reshape(GTOK, HEADS * HD)

def self_attention(queries, keys_all, values_all, table, segments):
    head_queries = split_heads(queries)
    head_keys = split_heads(keys_all)
    head_values = split_heads(values_all)
    bias_table = table.reshape(HEADS, BUCKETS)
    columns = jnp.arange(GTOK, dtype=jnp.int32)

    def one_block(row_start):
        rows = row_start + jnp.arange(BLK, dtype=jnp.int32)
        block_queries = lax.dynamic_slice_in_dim(head_queries, row_start, BLK, 1)
        scores = jnp.einsum('hqd,hkd->hqk', block_queries, head_keys, precision=lax.Precision.HIGHEST) * score_factor
        distance = rows[:, None] - columns[None, :]
        bias_grid = bias_table[:, bucket_of(jnp.maximum(distance, 0))]
        scores = low_back(scores + bias_grid)
        row_segments = lax.dynamic_slice_in_dim(segments, row_start, BLK)
        allowed = (distance >= 0) & (row_segments[:, None] == segments[None, :])
        scores = jnp.where(allowed[None], scores, masked_score)
        weights_now = jax.nn.softmax(scores, axis=-1)
        return jnp.einsum('hqk,hkd->hqd', low(weights_now), head_values, precision=lax.Precision.HIGHEST)
    starts = jnp.arange(GTOK // BLK, dtype=jnp.int32) * BLK
    return join_blocks(lax.map(jax.checkpoint(one_block), starts))

def cross_attention(queries, keys_all, values_all, segments):
    head_queries = split_heads(queries)
    head_keys = split_heads(keys_all)
    head_values = split_heads(values_all)
    key_seq = jnp.arange(ENC_G, dtype=jnp.int32) // ENC

    def one_block(row_start):
        block_queries = lax.dynamic_slice_in_dim(head_queries, row_start, BLK, 1)
        scores = jnp.einsum('hqd,hkd->hqk', block_queries, head_keys, precision=lax.Precision.HIGHEST) * score_factor
        scores = low_back(scores)
        row_segments = lax.dynamic_slice_in_dim(segments, row_start, BLK)
        allowed = row_segments[:, None] == key_seq[None, :]
        scores = jnp.where(allowed[None], scores, masked_score)
        weights_now = jax.nn.softmax(scores, axis=-1)
        return jnp.einsum('hqk,hkd->hqd', low(weights_now), head_values, precision=lax.Precision.HIGHEST)
    starts = jnp.arange(GTOK // BLK, dtype=jnp.int32) * BLK
    return join_blocks(lax.map(jax.checkpoint(one_block), starts))

def decoder_layer(given, states, params, segments):
    gain_one, self_in, self_out, table, gain_two, cross_query, cross_kv, cross_out, gain_three, gate_up, down_proj = params
    residual = low_back(given)
    normed_one = low(rms_scale(given, gain_one))
    projected = matmul(normed_one, self_in)
    queries = low_back(low(projected[:, :D]))
    keys_all = low_back(low(projected[:, D:2 * D]))
    values_all = low_back(low(projected[:, 2 * D:]))
    attended = low_back(low(self_attention(queries, keys_all, values_all, table, segments)))
    hidden_one = residual + low_back(matmul(attended, self_out))
    normed_two = low(rms_scale(hidden_one, gain_two))
    cross_queries = low_back(low(matmul(normed_two, cross_query)))
    state_proj = matmul(states, cross_kv)
    cross_keys = low_back(low(state_proj[:, :D]))
    cross_values = low_back(low(state_proj[:, D:]))
    crossed = low_back(low(cross_attention(cross_queries, cross_keys, cross_values, segments)))
    hidden_two = hidden_one + low_back(matmul(crossed, cross_out))
    normed_three = low(rms_scale(hidden_two, gain_three))
    gate_up_values = matmul(normed_three, gate_up)
    gate_part = low_back(gate_up_values[:, :FF])
    up_part = low_back(gate_up_values[:, FF:])
    activation = low(jax.nn.gelu(gate_part, approximate=True) * up_part)
    return hidden_two + matmul(activation, down_proj)

def reference(hidden_in, encoder_states, seq_lengths, deal, gain_self, w_self_in, w_self_out, rel_table, gain_cross, w_cross_q, w_cross_kv, w_cross_out, gain_ffn, w_gate_up, w_down, grad_out):
    weights = tuple((tensor.astype(jnp.float32) for tensor in (gain_self, w_self_in, w_self_out, rel_table, gain_cross, w_cross_q, w_cross_kv, w_cross_out, gain_ffn, w_gate_up, w_down)))

    def group_step(totals, item):
        dealt_in, states, lengths, dealing, cotangent = item
        segments = segment_ids(lengths, GTOK)
        inverse = jnp.argsort(dealing).astype(jnp.int32)

        def forward(dealt_values, state_values, params):
            given = jnp.take(dealt_values, inverse, axis=0)
            return decoder_layer(given, state_values, params, segments)
        output, pullback = jax.vjp(forward, dealt_in.astype(jnp.float32), states.astype(jnp.float32), weights)
        grad_dealt, grad_states, grad_params = pullback(cotangent.astype(jnp.float32))
        totals = jax.tree.map(lambda old_sum, new_term: old_sum + new_term, totals, grad_params)
        return (totals, (output.astype(jnp.bfloat16), grad_dealt.astype(jnp.bfloat16), grad_states.astype(jnp.bfloat16)))
    zeros = tuple((jnp.zeros(tensor.shape, jnp.float32) for tensor in weights))
    totals, (outputs, input_grads, state_grads) = lax.scan(group_step, zeros, (hidden_in, encoder_states, seq_lengths, deal, grad_out))
    return (outputs, input_grads, state_grads, totals[0], totals[1], totals[2], totals[3], totals[4], totals[5], totals[6], totals[7], totals[8], totals[9], totals[10])
```

```python
import jax
import jax.numpy as jnp
import numpy as np
from jax import lax
from jax.experimental import pallas as pl
from jax.experimental.pallas import tpu as pltpu
from jax.sharding import Mesh
from jax.sharding import PartitionSpec as P

HEADS = 16
HD = 64
BUCKETS = 32
ENC = 384


norm_eps = 1e-06
score_factor = 0.125
masked_score = -1e30
bucket_edges = [int(edge_value) for edge_value in np.ceil(16.0 * 8.0 ** (np.arange(1, 16) / 16.0))]


def bucket_of(distance):
    far_count = jnp.zeros_like(distance)
    for edge_value in bucket_edges:
        far_count = far_count + (distance >= edge_value).astype(jnp.int32)
    return jnp.where(distance < 16, distance, 16 + far_count)


def norm_apply(values, gain):
    inverse = lax.rsqrt(jnp.mean(values * values, axis=-1, keepdims=True) + norm_eps)
    return (values * inverse * gain, inverse)


def norm_back(values, inverse, gain, upstream):
    scaled = values * inverse
    gain_grad = jnp.sum(upstream * scaled, axis=0)
    inner_term = upstream * gain
    value_grad = inverse * (
        inner_term - scaled * jnp.mean(inner_term * scaled, axis=-1, keepdims=True)
    )
    return (value_grad, gain_grad)


def product(left, right):
    return jnp.dot(left, right, preferred_element_type=jnp.float32)


def product_tn(left, right):
    return lax.dot_general(
        left, right, (((0,), (0,)), ((), ())), preferred_element_type=jnp.float32
    )


def product_nt(left, right):
    return lax.dot_general(
        left, right, (((1,), (1,)), ((), ())), preferred_element_type=jnp.float32
    )


def toeplitz_grid(vector, block_len):
    reversed_vec = vector[:, ::-1]
    tiled = jnp.tile(reversed_vec, (1, block_len))
    window = tiled[:, block_len - 1 : block_len - 1 + block_len * (2 * block_len - 2)]
    return window.reshape(vector.shape[0], block_len, 2 * block_len - 2)[:, :, :block_len]


def toeplitz_back(score_grid, block_len):
    rows_here = score_grid.shape[0]
    widened = jnp.pad(score_grid, ((0, 0), (0, 0), (0, block_len - 2)))
    flattened = widened.reshape(rows_here, block_len * (2 * block_len - 2))
    flattened = jnp.pad(flattened, ((0, 0), (block_len - 1, 1)))
    folded = jnp.sum(flattened.reshape(rows_here, block_len, 2 * block_len - 1), axis=1)
    return folded[:, ::-1]


def masked_scores(queries, keys_all, pair_terms, query_size, key_size, query_block, key_block):
    query_part = lax.dynamic_slice_in_dim(queries, query_block * query_size, query_size, 0)
    key_part = lax.dynamic_slice_in_dim(keys_all, key_block * key_size, key_size, 0)
    scores = (
        jnp.einsum("qhd,khd->hqk", query_part, key_part, preferred_element_type=jnp.float32)
        * score_factor
    )
    bias_grid, allowed = pair_terms(query_block, key_block)
    return jnp.where(allowed[None], scores + bias_grid, masked_score)


def attend_forward(queries, keys_all, values_all, pair_terms, key_count, query_size, key_size):
    total_rows, heads_here, head_size = queries.shape

    def stats_step(query_block, lse_all):

        def stats_key_step(key_block, running):
            running_max, running_sum = running
            scores = masked_scores(
                queries, keys_all, pair_terms, query_size, key_size, query_block, key_block
            )
            new_max = jnp.maximum(running_max, jnp.max(scores, axis=-1))
            running_sum = running_sum * jnp.exp(running_max - new_max) + jnp.sum(
                jnp.exp(scores - new_max[:, :, None]), axis=-1
            )
            return (new_max, running_sum)

        initial = (
            jnp.full((heads_here, query_size), masked_score, jnp.float32),
            jnp.zeros((heads_here, query_size), jnp.float32),
        )
        running_max, running_sum = lax.fori_loop(0, key_count(query_block), stats_key_step, initial)
        block_lse = running_max + jnp.log(running_sum)
        return lax.dynamic_update_slice_in_dim(lse_all, block_lse, query_block * query_size, 1)

    lse_all = lax.fori_loop(
        0, total_rows // query_size, stats_step, jnp.zeros((heads_here, total_rows), jnp.float32)
    )

    def value_step(query_block, outputs):
        block_lse = lax.dynamic_slice_in_dim(lse_all, query_block * query_size, query_size, 1)

        def value_key_step(key_block, accum):
            scores = masked_scores(
                queries, keys_all, pair_terms, query_size, key_size, query_block, key_block
            )
            probabilities = jnp.exp(scores - block_lse[:, :, None]).astype(jnp.bfloat16)
            value_part = lax.dynamic_slice_in_dim(values_all, key_block * key_size, key_size, 0)
            return accum + jnp.einsum(
                "hqk,khd->qhd", probabilities, value_part, preferred_element_type=jnp.float32
            )

        accum = lax.fori_loop(
            0,
            key_count(query_block),
            value_key_step,
            jnp.zeros((query_size, heads_here, head_size), jnp.float32),
        )
        return lax.dynamic_update_slice_in_dim(outputs, accum, query_block * query_size, 0)

    outputs = lax.fori_loop(
        0, total_rows // query_size, value_step, jnp.zeros(queries.shape, jnp.float32)
    )
    return (outputs, lse_all)


def attend_backward(
    queries,
    keys_all,
    values_all,
    outputs,
    out_grads,
    lse_all,
    pair_terms,
    key_count,
    query_size,
    key_size,
    bias_back,
    bias_start,
):
    total_rows, heads_here, head_size = queries.shape
    delta_all = jnp.sum(out_grads.astype(jnp.float32) * outputs, axis=-1).T

    def query_step(query_block, outer_carry):
        key_grads, value_grads, query_grads, bias_accum = outer_carry
        row_start = query_block * query_size
        block_lse = lax.dynamic_slice_in_dim(lse_all, row_start, query_size, 1)
        block_delta = lax.dynamic_slice_in_dim(delta_all, row_start, query_size, 1)
        query_part = lax.dynamic_slice_in_dim(queries, row_start, query_size, 0)
        grad_part = lax.dynamic_slice_in_dim(out_grads, row_start, query_size, 0)

        def query_key_step(key_block, inner_carry):
            block_grad, key_grads, value_grads, bias_accum = inner_carry
            scores = masked_scores(
                queries, keys_all, pair_terms, query_size, key_size, query_block, key_block
            )
            probabilities = jnp.exp(scores - block_lse[:, :, None])
            offset = key_block * key_size
            key_part = lax.dynamic_slice_in_dim(keys_all, offset, key_size, 0)
            value_part = lax.dynamic_slice_in_dim(values_all, offset, key_size, 0)
            prob_grad = jnp.einsum(
                "qhd,khd->hqk", grad_part, value_part, preferred_element_type=jnp.float32
            )
            score_grad = (probabilities * (prob_grad - block_delta[:, :, None])).astype(
                jnp.bfloat16
            )
            block_grad = (
                block_grad
                + jnp.einsum(
                    "hqk,khd->qhd", score_grad, key_part, preferred_element_type=jnp.float32
                )
                * score_factor
            )
            key_add = (
                jnp.einsum(
                    "hqk,qhd->khd", score_grad, query_part, preferred_element_type=jnp.float32
                )
                * score_factor
            )
            value_add = jnp.einsum(
                "hqk,qhd->khd",
                probabilities.astype(jnp.bfloat16),
                grad_part,
                preferred_element_type=jnp.float32,
            )
            key_grads = lax.dynamic_update_slice_in_dim(
                key_grads,
                lax.dynamic_slice_in_dim(key_grads, offset, key_size, 0) + key_add,
                offset,
                0,
            )
            value_grads = lax.dynamic_update_slice_in_dim(
                value_grads,
                lax.dynamic_slice_in_dim(value_grads, offset, key_size, 0) + value_add,
                offset,
                0,
            )
            bias_accum = bias_back(bias_accum, query_block, key_block, score_grad)
            return (block_grad, key_grads, value_grads, bias_accum)

        initial = (
            jnp.zeros((query_size, heads_here, head_size), jnp.float32),
            key_grads,
            value_grads,
            bias_accum,
        )
        block_grad, key_grads, value_grads, bias_accum = lax.fori_loop(
            0, key_count(query_block), query_key_step, initial
        )
        query_grads = lax.dynamic_update_slice_in_dim(query_grads, block_grad, row_start, 0)
        return (key_grads, value_grads, query_grads, bias_accum)

    initial_state = (
        jnp.zeros(keys_all.shape, jnp.float32),
        jnp.zeros(values_all.shape, jnp.float32),
        jnp.zeros(queries.shape, jnp.float32),
        bias_start,
    )
    key_grads, value_grads, query_grads, bias_accum = lax.fori_loop(
        0, total_rows // query_size, query_step, initial_state
    )
    return (query_grads, key_grads, value_grads, bias_accum)


def per_device(
    hidden_in,
    encoder_states,
    seq_lengths,
    deal,
    gain_self,
    w_self_in,
    w_self_out,
    rel_table,
    gain_cross,
    w_cross_q,
    w_cross_kv,
    w_cross_out,
    gain_ffn,
    w_gate_up,
    w_down,
    grad_out,
):
    gathered = (
        lax.all_gather(gain_self, "fsdp", axis=0, tiled=True),
        lax.all_gather(w_self_in, "fsdp", axis=0, tiled=True),
        lax.all_gather(w_self_out, "fsdp", axis=0, tiled=True),
        lax.all_gather(rel_table, "fsdp", axis=0, tiled=True),
        lax.all_gather(gain_cross, "fsdp", axis=0, tiled=True),
        lax.all_gather(w_cross_q, "fsdp", axis=0, tiled=True),
        lax.all_gather(w_cross_kv, "fsdp", axis=0, tiled=True),
        lax.all_gather(w_cross_out, "fsdp", axis=0, tiled=True),
        lax.all_gather(gain_ffn, "fsdp", axis=0, tiled=True),
        lax.all_gather(w_gate_up, "fsdp", axis=0, tiled=True),
        lax.all_gather(w_down, "fsdp", axis=0, tiled=True),
    )
    (
        gain_one,
        self_in,
        self_out,
        table_flat,
        gain_two,
        cross_query,
        cross_kv,
        cross_out,
        gain_three,
        gate_up,
        down_proj,
    ) = gathered
    tokens = hidden_in[0]
    states = encoder_states[0]
    lengths = seq_lengths[0]
    dealing = deal[0]
    cotangent = grad_out[0]
    seq_count = lax.axis_size("seq")
    heads_here = HEADS // seq_count
    model_width = tokens.shape[1]
    hidden_units = down_proj.shape[0]
    total_rows = dealing.shape[0]
    state_rows = states.shape[0] * seq_count
    block_size = min(512, total_rows)
    key_size = min(512, state_rows)
    inverse = jnp.argsort(dealing)
    seq_ends = jnp.cumsum(lengths)
    places = jnp.arange(total_rows, dtype=jnp.int32)
    segments = jnp.sum((places[:, None] >= seq_ends[None, :]).astype(jnp.int32), axis=1)
    state_seq = jnp.arange(state_rows, dtype=jnp.int32) // ENC
    head_start = lax.axis_index("seq") * heads_here
    table_here = lax.dynamic_slice_in_dim(
        table_flat.astype(jnp.float32).reshape(HEADS, BUCKETS), head_start, heads_here, 0
    )
    one_hot = (bucket_of(places)[None, :] == jnp.arange(BUCKETS, dtype=jnp.int32)[:, None]).astype(
        jnp.float32
    )
    rel_bias = jnp.dot(table_here, one_hot, precision=lax.Precision.HIGHEST)
    rel_pad = jnp.pad(rel_bias, ((0, 0), (block_size - 1, block_size)))

    def self_pairs(query_block, key_block):
        rows = query_block * block_size + jnp.arange(block_size, dtype=jnp.int32)
        columns = key_block * block_size + jnp.arange(block_size, dtype=jnp.int32)
        row_segments = lax.dynamic_slice_in_dim(segments, query_block * block_size, block_size)
        column_segments = lax.dynamic_slice_in_dim(segments, key_block * block_size, block_size)
        allowed = (rows[:, None] >= columns[None, :]) & (
            row_segments[:, None] == column_segments[None, :]
        )
        vector = lax.dynamic_slice_in_dim(
            rel_pad, (query_block - key_block) * block_size, 2 * block_size - 1, 1
        )
        return (toeplitz_grid(vector, block_size), allowed)

    def self_bias_back(bias_accum, query_block, key_block, score_grad):
        offset = (query_block - key_block) * block_size
        folded = toeplitz_back(score_grad.astype(jnp.float32), block_size)
        updated = lax.dynamic_slice_in_dim(bias_accum, offset, 2 * block_size - 1, 1) + folded
        return lax.dynamic_update_slice_in_dim(bias_accum, updated, offset, 1)

    def cross_pairs(query_block, key_block):
        row_segments = lax.dynamic_slice_in_dim(segments, query_block * block_size, block_size)
        key_segments = lax.dynamic_slice_in_dim(state_seq, key_block * key_size, key_size)
        return (jnp.zeros((), jnp.float32), row_segments[:, None] == key_segments[None, :])

    def cross_bias_back(bias_accum, query_block, key_block, score_grad):
        return bias_accum

    def self_keys(query_block):
        return query_block + 1

    def cross_keys(query_block):
        return state_rows // key_size

    def to_heads(values):
        return values.reshape(values.shape[0], heads_here, HD)

    token_values = tokens.astype(jnp.float32)
    normed_one, inverse_one = norm_apply(token_values, gain_one.astype(jnp.float32))
    normed_one = normed_one.astype(jnp.bfloat16)
    projected = product(normed_one, self_in).astype(jnp.bfloat16)
    query_heads, key_heads, value_heads, token_heads = (
        lax.all_to_all(projected[:, :model_width], "seq", split_axis=1, concat_axis=0, tiled=True),
        lax.all_to_all(
            projected[:, model_width : 2 * model_width],
            "seq",
            split_axis=1,
            concat_axis=0,
            tiled=True,
        ),
        lax.all_to_all(
            projected[:, 2 * model_width :], "seq", split_axis=1, concat_axis=0, tiled=True
        ),
        lax.all_to_all(tokens, "seq", split_axis=1, concat_axis=0, tiled=True),
    )
    query_given = to_heads(jnp.take(query_heads, inverse, axis=0))
    key_given = to_heads(jnp.take(key_heads, inverse, axis=0))
    value_given = to_heads(jnp.take(value_heads, inverse, axis=0))
    token_given = jnp.take(token_heads, inverse, axis=0)
    self_result, self_lse = attend_forward(
        query_given, key_given, value_given, self_pairs, self_keys, block_size, block_size
    )
    self_low = self_result.astype(jnp.bfloat16).reshape(total_rows, heads_here * HD)
    attended_tok, residual_tok = (
        lax.all_to_all(self_low, "seq", split_axis=0, concat_axis=1, tiled=True),
        lax.all_to_all(token_given, "seq", split_axis=0, concat_axis=1, tiled=True),
    )
    hidden_one = residual_tok.astype(jnp.float32) + product(attended_tok, self_out)
    normed_two, inverse_two = norm_apply(hidden_one, gain_two.astype(jnp.float32))
    normed_two = normed_two.astype(jnp.bfloat16)
    cross_query_tok = product(normed_two, cross_query).astype(jnp.bfloat16)
    state_proj = product(states, cross_kv).astype(jnp.bfloat16)
    cross_query_heads, cross_key_heads, cross_value_heads = (
        lax.all_to_all(cross_query_tok, "seq", split_axis=1, concat_axis=0, tiled=True),
        lax.all_to_all(state_proj[:, :model_width], "seq", split_axis=1, concat_axis=0, tiled=True),
        lax.all_to_all(state_proj[:, model_width:], "seq", split_axis=1, concat_axis=0, tiled=True),
    )
    cross_queries = to_heads(cross_query_heads)
    cross_keys_all = to_heads(cross_key_heads)
    cross_values_all = to_heads(cross_value_heads)
    cross_result, cross_lse = attend_forward(
        cross_queries,
        cross_keys_all,
        cross_values_all,
        cross_pairs,
        cross_keys,
        block_size,
        key_size,
    )
    cross_low = cross_result.astype(jnp.bfloat16).reshape(total_rows, heads_here * HD)
    crossed_tok = lax.all_to_all(cross_low, "seq", split_axis=0, concat_axis=1, tiled=True)
    hidden_two = hidden_one + product(crossed_tok, cross_out)
    normed_three, inverse_three = norm_apply(hidden_two, gain_three.astype(jnp.float32))
    normed_three = normed_three.astype(jnp.bfloat16)
    gate_up_values = product(normed_three, gate_up)
    gate_part = gate_up_values[:, :hidden_units]
    up_part = gate_up_values[:, hidden_units:]
    gelu_values, gelu_pull = jax.vjp(
        lambda gate_values: jax.nn.gelu(gate_values, approximate=True), gate_part
    )
    activation = (gelu_values * up_part).astype(jnp.bfloat16)
    block_result = (hidden_two + product(activation, down_proj)).astype(jnp.bfloat16)
    (
        gain_one_b,
        self_in_b,
        self_out_b,
        table_flat_b,
        gain_two_b,
        cross_query_b,
        cross_kv_b,
        cross_out_b,
        gain_three_b,
        gate_up_b,
        down_proj_b,
    ) = gathered
    upstream = cotangent.astype(jnp.float32)
    grad_down = product_tn(activation, cotangent)
    act_grad = product_nt(cotangent, down_proj_b)
    gate_grad = gelu_pull(act_grad * up_part)[0]
    up_grad = act_grad * gelu_values
    gate_up_grad = jnp.concatenate([gate_grad, up_grad], axis=1).astype(jnp.bfloat16)
    grad_gate_up = product_tn(normed_three, gate_up_grad)
    normed_three_grad = product_nt(gate_up_grad, gate_up_b)
    hidden_two_part, grad_gain_three = norm_back(
        hidden_two, inverse_three, gain_three_b.astype(jnp.float32), normed_three_grad
    )
    hidden_two_grad = upstream + hidden_two_part
    second_low = hidden_two_grad.astype(jnp.bfloat16)
    grad_cross_out = product_tn(crossed_tok, second_low)
    crossed_grad = product_nt(second_low, cross_out_b).astype(jnp.bfloat16)
    crossed_grad_heads = lax.all_to_all(
        crossed_grad, "seq", split_axis=1, concat_axis=0, tiled=True
    )
    cq_grad, ck_grad, cv_grad, unused_bias = attend_backward(
        cross_queries,
        cross_keys_all,
        cross_values_all,
        cross_result,
        to_heads(crossed_grad_heads),
        cross_lse,
        cross_pairs,
        cross_keys,
        block_size,
        key_size,
        cross_bias_back,
        jnp.zeros((), jnp.float32),
    )
    cq_tok, ck_tok, cv_tok = (
        lax.all_to_all(
            cq_grad.astype(jnp.bfloat16).reshape(total_rows, heads_here * HD),
            "seq",
            split_axis=0,
            concat_axis=1,
            tiled=True,
        ),
        lax.all_to_all(
            ck_grad.astype(jnp.bfloat16).reshape(state_rows, heads_here * HD),
            "seq",
            split_axis=0,
            concat_axis=1,
            tiled=True,
        ),
        lax.all_to_all(
            cv_grad.astype(jnp.bfloat16).reshape(state_rows, heads_here * HD),
            "seq",
            split_axis=0,
            concat_axis=1,
            tiled=True,
        ),
    )
    grad_cross_query = product_tn(normed_two, cq_tok)
    state_grad_rows = jnp.concatenate([ck_tok, cv_tok], axis=1)
    grad_cross_kv = product_tn(states, state_grad_rows)
    state_grad = product_nt(state_grad_rows, cross_kv_b).astype(jnp.bfloat16)
    normed_two_grad = product_nt(cq_tok, cross_query_b)
    hidden_one_part, grad_gain_two = norm_back(
        hidden_one, inverse_two, gain_two_b.astype(jnp.float32), normed_two_grad
    )
    hidden_one_grad = hidden_two_grad + hidden_one_part
    first_low = hidden_one_grad.astype(jnp.bfloat16)
    grad_self_out = product_tn(attended_tok, first_low)
    attended_grad = product_nt(first_low, self_out_b).astype(jnp.bfloat16)
    attended_grad_heads, residual_grad_heads = (
        lax.all_to_all(attended_grad, "seq", split_axis=1, concat_axis=0, tiled=True),
        lax.all_to_all(first_low, "seq", split_axis=1, concat_axis=0, tiled=True),
    )
    bias_start = jnp.zeros(rel_pad.shape, jnp.float32)
    sq_grad, sk_grad, sv_grad, bias_accum = attend_backward(
        query_given,
        key_given,
        value_given,
        self_result,
        to_heads(attended_grad_heads),
        self_lse,
        self_pairs,
        self_keys,
        block_size,
        block_size,
        self_bias_back,
        bias_start,
    )
    query_dealt = jnp.take(
        sq_grad.astype(jnp.bfloat16).reshape(total_rows, heads_here * HD), dealing, axis=0
    )
    key_dealt = jnp.take(
        sk_grad.astype(jnp.bfloat16).reshape(total_rows, heads_here * HD), dealing, axis=0
    )
    value_dealt = jnp.take(
        sv_grad.astype(jnp.bfloat16).reshape(total_rows, heads_here * HD), dealing, axis=0
    )
    residual_dealt = jnp.take(residual_grad_heads, dealing, axis=0)
    q_tok, k_tok, v_tok, residual_back = (
        lax.all_to_all(query_dealt, "seq", split_axis=0, concat_axis=1, tiled=True),
        lax.all_to_all(key_dealt, "seq", split_axis=0, concat_axis=1, tiled=True),
        lax.all_to_all(value_dealt, "seq", split_axis=0, concat_axis=1, tiled=True),
        lax.all_to_all(residual_dealt, "seq", split_axis=0, concat_axis=1, tiled=True),
    )
    projected_grad = jnp.concatenate([q_tok, k_tok, v_tok], axis=1)
    grad_self_in = product_tn(normed_one, projected_grad)
    normed_one_grad = product_nt(projected_grad, self_in_b)
    token_part, grad_gain_one = norm_back(
        token_values, inverse_one, gain_one_b.astype(jnp.float32), normed_one_grad
    )
    input_result = (residual_back.astype(jnp.float32) + token_part).astype(jnp.bfloat16)
    distance_grad = lax.dynamic_slice_in_dim(bias_accum, block_size - 1, total_rows, 1)
    table_grad_here = jnp.dot(distance_grad, one_hot.T, precision=lax.Precision.HIGHEST)
    grad_table = lax.dynamic_update_slice_in_dim(
        jnp.zeros((HEADS, BUCKETS), jnp.float32), table_grad_here, head_start, 0
    ).reshape(HEADS * BUCKETS)
    summed = (
        lax.psum_scatter(grad_gain_one, ("seq", "fsdp"), scatter_dimension=0, tiled=True),
        lax.psum_scatter(grad_self_in, ("seq", "fsdp"), scatter_dimension=0, tiled=True),
        lax.psum_scatter(grad_self_out, ("seq", "fsdp"), scatter_dimension=0, tiled=True),
        lax.psum_scatter(grad_table, ("seq", "fsdp"), scatter_dimension=0, tiled=True),
        lax.psum_scatter(grad_gain_two, ("seq", "fsdp"), scatter_dimension=0, tiled=True),
        lax.psum_scatter(grad_cross_query, ("seq", "fsdp"), scatter_dimension=0, tiled=True),
        lax.psum_scatter(grad_cross_kv, ("seq", "fsdp"), scatter_dimension=0, tiled=True),
        lax.psum_scatter(grad_cross_out, ("seq", "fsdp"), scatter_dimension=0, tiled=True),
        lax.psum_scatter(grad_gain_three, ("seq", "fsdp"), scatter_dimension=0, tiled=True),
        lax.psum_scatter(grad_gate_up, ("seq", "fsdp"), scatter_dimension=0, tiled=True),
        lax.psum_scatter(grad_down, ("seq", "fsdp"), scatter_dimension=0, tiled=True),
    )
    reduced = (
        lax.psum(summed[0].astype(jnp.bfloat16), "rep").astype(jnp.float32),
        lax.psum(summed[1].astype(jnp.bfloat16), "rep").astype(jnp.float32),
        lax.psum(summed[2].astype(jnp.bfloat16), "rep").astype(jnp.float32),
        lax.psum(summed[3].astype(jnp.bfloat16), "rep").astype(jnp.float32),
        lax.psum(summed[4].astype(jnp.bfloat16), "rep").astype(jnp.float32),
        lax.psum(summed[5].astype(jnp.bfloat16), "rep").astype(jnp.float32),
        lax.psum(summed[6].astype(jnp.bfloat16), "rep").astype(jnp.float32),
        lax.psum(summed[7].astype(jnp.bfloat16), "rep").astype(jnp.float32),
        lax.psum(summed[8].astype(jnp.bfloat16), "rep").astype(jnp.float32),
        lax.psum(summed[9].astype(jnp.bfloat16), "rep").astype(jnp.float32),
        lax.psum(summed[10].astype(jnp.bfloat16), "rep").astype(jnp.float32),
    )
    return (
        block_result[None],
        input_result[None],
        state_grad[None],
        reduced[0],
        reduced[1],
        reduced[2],
        reduced[3],
        reduced[4],
        reduced[5],
        reduced[6],
        reduced[7],
        reduced[8],
        reduced[9],
        reduced[10],
    )


AXES = ("seq", "fsdp", "rx", "core")
TILE = 128


def axis_spots():
    return tuple(lax.axis_index(name) for name in AXES)


def shift_devices(values, mapping):
    sizes = [lax.axis_size(name) for name in AXES]
    pairs = []
    for place in np.ndindex(*sizes):
        target = mapping(*place)
        pairs.append(
            (int(np.ravel_multi_index(place, sizes)), int(np.ravel_multi_index(target, sizes)))
        )
    return lax.ppermute(values, AXES, pairs)


def swap_core(values):
    return shift_devices(values, lambda y, z, x, c: (y, z, x, 1 - c))


def swap_x(values):
    return shift_devices(values, lambda y, z, x, c: (y, z, 1 - x, c))


def swap_y(values):
    return shift_devices(values, lambda y, z, x, c: (1 - y, z, x, c))


def shift_z(values, step):
    count = lax.axis_size("fsdp")
    return shift_devices(values, lambda y, z, x, c: (y, (z + step) % count, x, c))


def to_worker(values):
    return shift_devices(values, lambda y, z, x, c: (c, z, x, y))


def ordered(spot, mine, other):
    return (jnp.where(spot == 0, mine, other), jnp.where(spot == 0, other, mine))


def join(spot, mine, other, axis):
    return jnp.concatenate(ordered(spot, mine, other), axis=axis)


def cut(values, spot, size, axis):
    return lax.dynamic_slice_in_dim(values, spot * size, size, axis)


def gather_blocks(block, x_first, axis):
    y, z, x, c = axis_spots()
    count = lax.axis_size("fsdp")
    size = block.shape[axis]
    outer, inner = (y, x) if x_first else (x, y)
    inner_swap, outer_swap = (swap_x, swap_y) if x_first else (swap_y, swap_x)
    piece = lax.dynamic_slice_in_dim(
        block, outer * (size // 2) + inner * (size // 4), size // 4, axis
    )
    rows = block.shape[0]
    whole = jnp.zeros((count * rows,) + block.shape[1:], block.dtype)
    whole = lax.dynamic_update_slice_in_dim(whole, block, z * rows, 0)
    for step in range(1, count):
        held = shift_z(piece, step)
        held = join(inner, held, inner_swap(held), axis)
        held = join(outer, held, outer_swap(held), axis)
        source = lax.rem(z + count - step, count)
        whole = lax.dynamic_update_slice_in_dim(whole, held, source * rows, 0)
    return whole


def own_rows_of(gathered, blocks):
    c = lax.axis_index("core")
    half = blocks // 2
    parts = gathered.reshape((blocks, gathered.shape[0] // blocks) + gathered.shape[1:])
    mine = cut(parts, c, half, 0)
    other = swap_core(cut(parts, 1 - c, half, 0))
    return join(c, mine, other, 1).reshape((-1,) + gathered.shape[1:])


def spread_rows(grad, blocks):
    c = lax.axis_index("core")
    half = blocks // 2
    rows = grad.shape[0] // half
    parts = grad.reshape(half, 2, rows // 2, grad.shape[1])
    mine = cut(parts, c, 1, 1)[:, 0]
    other = swap_core(cut(parts, 1 - c, 1, 1)[:, 0])
    return join(c, mine, other, 0)


def add_low(mine, other):
    return (mine.astype(jnp.float32) + other.astype(jnp.float32)).astype(jnp.bfloat16)


def reduce_blocks(grad):
    y, z, x, c = axis_spots()
    blocks, rows, columns = grad.shape
    count = lax.axis_size("fsdp")

    def x_step(part):
        half = part.shape[2] // 2
        return add_low(cut(part, x, half, 2), swap_x(cut(part, 1 - x, half, 2)))

    def y_step(part):
        half = part.shape[0] // 2
        return add_low(cut(part, y, half, 0), swap_y(cut(part, 1 - y, half, 0)))

    def z_step(part):
        total = cut(part, z, 1, 0)[0].astype(jnp.float32)
        for step in range(1, count):
            target = lax.rem(z + step, count)
            total = total + shift_z(cut(part, target, 1, 0)[0], step).astype(jnp.float32)
        return total.astype(jnp.bfloat16)

    first = (columns // 2 + 255) // 256 * 256
    left = z_step(y_step(x_step(grad[:, :, :first])))
    right = z_step(x_step(y_step(grad[:, :, first:])))
    mine = jnp.concatenate([left, right], axis=1)
    low, high = ordered(x, mine, swap_x(mine))
    cut_at = left.shape[1]
    full = jnp.concatenate(
        [low[:, :cut_at], high[:, :cut_at], low[:, cut_at:], high[:, cut_at:]], axis=1
    )
    return ordered(c, full, swap_core(full))


def column_result(low, high, pieces):
    width = low.shape[1] // pieces
    parts = []
    for piece in range(pieces):
        parts.append(low[:, piece * width : (piece + 1) * width])
        parts.append(high[:, piece * width : (piece + 1) * width])
    return jnp.concatenate(parts, axis=1).astype(jnp.float32)


def row_result(low, high):
    return jnp.concatenate([low, high], axis=0).astype(jnp.float32)


def dot_nn(left, right):
    return lax.dot_general(
        left, right, (((1,), (0,)), ((), ())), preferred_element_type=jnp.float32
    )


def dot_nt(left, right):
    return lax.dot_general(
        left, right, (((1,), (1,)), ((), ())), preferred_element_type=jnp.float32
    )


def dot_tn(left, right):
    return lax.dot_general(
        left, right, (((0,), (0,)), ((), ())), preferred_element_type=jnp.float32
    )


def half_lanes(values, side):
    lanes = lax.broadcasted_iota(jnp.int32, values.shape, 1)
    inside = (lanes >= side * HD) & (lanes < (side + 1) * HD)
    return jnp.where(inside, values, jnp.zeros_like(values))


def pair_lanes(left, right, rows):
    lanes = lax.broadcasted_iota(jnp.int32, (rows, 2 * HD), 1)
    return jnp.where(lanes < HD, left, right)


def fill_bias(bias_ref, table_ref, head, buckets, distance):
    far = table_ref[head, BUCKETS - 1]
    near = jnp.full(buckets.shape, far, jnp.float32)
    for bucket in range(BUCKETS - 1):
        near = jnp.where(buckets == bucket, table_ref[head, bucket], near)
    near = jnp.where(distance < 0, masked_score, near)
    width = bias_ref.shape[1]
    bias_ref[:, : width - 2 * TILE] = jnp.full((TILE, width - 2 * TILE), far, jnp.float32)
    bias_ref[:, width - 2 * TILE :] = near


def near_buckets():
    rows = lax.broadcasted_iota(jnp.int32, (TILE, 2 * TILE), 0)
    columns = lax.broadcasted_iota(jnp.int32, (TILE, 2 * TILE), 1)
    distance = TILE + rows - columns
    return (distance, bucket_of(distance))


def self_scores(query, keys, bias_ref, starts, row):
    size = row + TILE
    width = bias_ref.shape[1]
    scores = dot_nt(query, keys[:size]) + bias_ref[:, width - size :]
    columns = lax.broadcasted_iota(jnp.int32, (TILE, size), 1)
    return jnp.where(columns >= starts, scores, masked_score)


def self_forward_body(table_ref, start_ref, q_ref, k_ref, v_ref, o_ref, lse_ref, bias_ref):
    pair = pl.program_id(0)
    total = q_ref.shape[0]
    distance, buckets = near_buckets()
    keys = k_ref[...]
    outs = {}
    for side in range(2):
        fill_bias(bias_ref, table_ref, 2 * pair + side, buckets, distance)
        query = half_lanes(q_ref[...], side) * jnp.asarray(score_factor, jnp.bfloat16)
        values = half_lanes(v_ref[...], side)
        for row in range(0, total, TILE):
            scores = self_scores(
                query[row : row + TILE], keys, bias_ref, start_ref[row : row + TILE, :], row
            )
            top = jnp.max(scores, axis=-1, keepdims=True)
            weights = jnp.exp(scores - top)
            mass = jnp.sum(weights, axis=-1, keepdims=True)
            low = (weights / mass).astype(jnp.bfloat16)
            outs[side, row] = (dot_nn(low, values[: row + TILE]), top + jnp.log(mass))
    for row in range(0, total, TILE):
        o_ref[row : row + TILE, :] = (outs[0, row][0] + outs[1, row][0]).astype(jnp.bfloat16)
        lse_ref[row : row + TILE, :] = pair_lanes(outs[0, row][1], outs[1, row][1], TILE)


def self_backward_body(
    table_ref,
    start_ref,
    q_ref,
    k_ref,
    v_ref,
    g_ref,
    lse_ref,
    dq_ref,
    dk_ref,
    dv_ref,
    table_grad_ref,
    bias_ref,
    fold_ref,
    dk_sum,
    dv_sum,
):
    pair = pl.program_id(0)
    total = q_ref.shape[0]
    distance, buckets = near_buckets()
    keys = k_ref[...]
    values = v_ref[...]
    width = bias_ref.shape[1]
    dk_sum[...] = jnp.zeros_like(dk_sum)
    dv_sum[...] = jnp.zeros_like(dv_sum)
    dq_parts = {}
    for side in range(2):
        fill_bias(bias_ref, table_ref, 2 * pair + side, buckets, distance)
        fold_ref[...] = jnp.zeros_like(fold_ref)
        query = half_lanes(q_ref[...], side) * jnp.asarray(score_factor, jnp.bfloat16)
        grads = half_lanes(g_ref[...], side)
        side_keys = half_lanes(keys, side)
        for row in range(0, total, TILE):
            size = row + TILE
            rows = slice(row, size)
            scores = self_scores(query[rows], keys, bias_ref, start_ref[rows, :], row)
            weights = jnp.exp(scores - lse_ref[rows, side * HD : side * HD + 1])
            grad_weights = dot_nt(grads[rows], values[:size])
            delta = jnp.sum(weights * grad_weights, axis=-1, keepdims=True)
            grad_scores = weights * (grad_weights - delta)
            fold_ref[:, width - size :] = fold_ref[:, width - size :] + grad_scores
            low = grad_scores.astype(jnp.bfloat16)
            dq_parts[side, row] = dot_nn(low, side_keys[:size]) * score_factor
            dk_sum[:size, :] = dk_sum[:size, :] + dot_tn(low, query[rows])
            dv_sum[:size, :] = dv_sum[:size, :] + dot_tn(weights.astype(jnp.bfloat16), grads[rows])
        near = fold_ref[:, width - 2 * TILE :]
        far = jnp.sum(fold_ref[:, : width - 2 * TILE], axis=0, keepdims=True)
        for bucket in range(BUCKETS):
            line = jnp.sum(jnp.where(buckets == bucket, near, 0.0), axis=0, keepdims=True)
            line = line[:, :TILE] + line[:, TILE:]
            if bucket == BUCKETS - 1:
                for at in range(0, width - 2 * TILE, TILE):
                    line = line + far[:, at : at + TILE]
            table_grad_ref[0, side, bucket : bucket + 1, :] = line
    for row in range(0, total, TILE):
        dq_ref[row : row + TILE, :] = (dq_parts[0, row] + dq_parts[1, row]).astype(jnp.bfloat16)
    dk_ref[...] = dk_sum[...].astype(jnp.bfloat16)
    dv_ref[...] = dv_sum[...].astype(jnp.bfloat16)


def pair_block(rows, offset):
    return pl.BlockSpec((rows, 2 * HD), lambda pair: (0, pair + offset))


def self_forward(projected, table, starts):
    total, width = projected.shape
    heads_here = width // (3 * HD)
    pairs = heads_here // 2
    return pl.pallas_call(
        self_forward_body,
        grid=(pairs,),
        in_specs=[
            pl.BlockSpec(memory_space=pltpu.SMEM),
            pl.BlockSpec((total, 1), lambda pair: (0, 0)),
            pair_block(total, 0),
            pair_block(total, pairs),
            pair_block(total, 2 * pairs),
        ],
        out_specs=[pair_block(total, 0), pair_block(total, 0)],
        out_shape=[
            jax.ShapeDtypeStruct((total, heads_here * HD), jnp.bfloat16),
            jax.ShapeDtypeStruct((total, heads_here * HD), jnp.float32),
        ],
        scratch_shapes=[pltpu.VMEM((TILE, total), jnp.float32)],
        cost_estimate=pl.CostEstimate(
            flops=4 * total * total * HD * heads_here,
            bytes_accessed=12 * total * heads_here * HD,
            transcendentals=total * total * heads_here,
        ),
        name="self_forward",
    )(table, starts, projected, projected, projected)


def self_backward(projected, out_grads, lse, table, starts):
    total, width = projected.shape
    heads_here = width // (3 * HD)
    pairs = heads_here // 2
    one = jax.ShapeDtypeStruct((total, heads_here * HD), jnp.bfloat16)
    return pl.pallas_call(
        self_backward_body,
        grid=(pairs,),
        in_specs=[
            pl.BlockSpec(memory_space=pltpu.SMEM),
            pl.BlockSpec((total, 1), lambda pair: (0, 0)),
            pair_block(total, 0),
            pair_block(total, pairs),
            pair_block(total, 2 * pairs),
            pair_block(total, 0),
            pair_block(total, 0),
        ],
        out_specs=[
            pair_block(total, 0),
            pair_block(total, 0),
            pair_block(total, 0),
            pl.BlockSpec((1, 2, BUCKETS, TILE), lambda pair: (pair, 0, 0, 0)),
        ],
        out_shape=[
            one,
            one,
            one,
            jax.ShapeDtypeStruct((pairs, 2, BUCKETS, TILE), jnp.float32),
        ],
        scratch_shapes=[
            pltpu.VMEM((TILE, total), jnp.float32),
            pltpu.VMEM((TILE, total), jnp.float32),
            pltpu.VMEM((total, 2 * HD), jnp.float32),
            pltpu.VMEM((total, 2 * HD), jnp.float32),
        ],
        cost_estimate=pl.CostEstimate(
            flops=10 * total * total * HD * heads_here,
            bytes_accessed=20 * total * heads_here * HD,
            transcendentals=total * total * heads_here,
        ),
        name="self_backward",
    )(table, starts, projected, projected, projected, out_grads, lse)


def meets(bound_ref, seq, row):
    return (bound_ref[seq] < row + TILE) & (bound_ref[seq + 1] > row)


def cross_forward_body(bound_ref, seg_ref, q_ref, k_ref, v_ref, o_ref, lse_ref):
    total = q_ref.shape[0]
    seq_count = k_ref.shape[0] // ENC
    for row in range(0, total, TILE):
        rows = slice(row, row + TILE)
        for seq in range(seq_count):

            @pl.when(meets(bound_ref, seq, row))
            def one_pair(rows=rows, seq=seq):
                keys = k_ref[seq * ENC : (seq + 1) * ENC, :]
                values = v_ref[seq * ENC : (seq + 1) * ENC, :]
                result = jnp.zeros((TILE, 2 * HD), jnp.float32)
                tops = []
                for side in range(2):
                    query = half_lanes(q_ref[rows, :], side) * jnp.asarray(
                        score_factor, jnp.bfloat16
                    )
                    scores = dot_nt(query, keys)
                    top = jnp.max(scores, axis=-1, keepdims=True)
                    weights = jnp.exp(scores - top)
                    mass = jnp.sum(weights, axis=-1, keepdims=True)
                    low = (weights / mass).astype(jnp.bfloat16)
                    result = result + dot_nn(low, half_lanes(values, side))
                    tops.append(top + jnp.log(mass))
                chosen = seg_ref[rows, :] == seq
                o_ref[rows, :] = jnp.where(chosen, result.astype(jnp.bfloat16), o_ref[rows, :])
                lse_ref[rows, :] = jnp.where(
                    chosen, pair_lanes(tops[0], tops[1], TILE), lse_ref[rows, :]
                )


def cross_backward_body(
    bound_ref,
    seg_ref,
    q_ref,
    k_ref,
    v_ref,
    g_ref,
    lse_ref,
    dq_ref,
    dk_ref,
    dv_ref,
    dq_sum,
    dk_sum,
    dv_sum,
):
    total = q_ref.shape[0]
    seq_count = k_ref.shape[0] // ENC
    dq_sum[...] = jnp.zeros_like(dq_sum)
    dk_sum[...] = jnp.zeros_like(dk_sum)
    dv_sum[...] = jnp.zeros_like(dv_sum)
    for row in range(0, total, TILE):
        rows = slice(row, row + TILE)
        for seq in range(seq_count):

            @pl.when(meets(bound_ref, seq, row))
            def one_pair(rows=rows, seq=seq):
                spot = slice(seq * ENC, (seq + 1) * ENC)
                keys = k_ref[spot, :]
                values = v_ref[spot, :]
                chosen = seg_ref[rows, :] == seq
                for side in range(2):
                    query = half_lanes(q_ref[rows, :], side) * jnp.asarray(
                        score_factor, jnp.bfloat16
                    )
                    grads = half_lanes(g_ref[rows, :], side)
                    scores = dot_nt(query, keys)
                    weights = jnp.exp(scores - lse_ref[rows, side * HD : side * HD + 1])
                    weights = jnp.where(chosen, weights, 0.0)
                    grad_weights = dot_nt(grads, values)
                    delta = jnp.sum(weights * grad_weights, axis=-1, keepdims=True)
                    low = (weights * (grad_weights - delta)).astype(jnp.bfloat16)
                    dq_sum[rows, :] = (
                        dq_sum[rows, :] + dot_nn(low, half_lanes(keys, side)) * score_factor
                    )
                    dk_sum[spot, :] = dk_sum[spot, :] + dot_tn(low, query)
                    dv_sum[spot, :] = dv_sum[spot, :] + dot_tn(weights.astype(jnp.bfloat16), grads)

    dq_ref[...] = dq_sum[...].astype(jnp.bfloat16)
    dk_ref[...] = dk_sum[...].astype(jnp.bfloat16)
    dv_ref[...] = dv_sum[...].astype(jnp.bfloat16)


def cross_forward(queries, state_proj, bounds, segments):
    total, width = queries.shape
    state_rows = state_proj.shape[0]
    pairs = width // (2 * HD)
    return pl.pallas_call(
        cross_forward_body,
        grid=(pairs,),
        in_specs=[
            pl.BlockSpec(memory_space=pltpu.SMEM),
            pl.BlockSpec((total, 1), lambda pair: (0, 0)),
            pair_block(total, 0),
            pair_block(state_rows, 0),
            pair_block(state_rows, pairs),
        ],
        out_specs=[pair_block(total, 0), pair_block(total, 0)],
        out_shape=[
            jax.ShapeDtypeStruct((total, width), jnp.bfloat16),
            jax.ShapeDtypeStruct((total, width), jnp.float32),
        ],
        cost_estimate=pl.CostEstimate(
            flops=4 * total * ENC * width * 2,
            bytes_accessed=8 * total * width + 4 * state_rows * width,
            transcendentals=2 * total * ENC * width // HD,
        ),
        name="cross_forward",
    )(bounds, segments, queries, state_proj, state_proj)


def cross_backward(queries, state_proj, out_grads, lse, bounds, segments):
    total, width = queries.shape
    state_rows = state_proj.shape[0]
    pairs = width // (2 * HD)
    return pl.pallas_call(
        cross_backward_body,
        grid=(pairs,),
        in_specs=[
            pl.BlockSpec(memory_space=pltpu.SMEM),
            pl.BlockSpec((total, 1), lambda pair: (0, 0)),
            pair_block(total, 0),
            pair_block(state_rows, 0),
            pair_block(state_rows, pairs),
            pair_block(total, 0),
            pair_block(total, 0),
        ],
        out_specs=[pair_block(total, 0), pair_block(state_rows, 0), pair_block(state_rows, 0)],
        out_shape=[
            jax.ShapeDtypeStruct((total, width), jnp.bfloat16),
            jax.ShapeDtypeStruct((state_rows, width), jnp.bfloat16),
            jax.ShapeDtypeStruct((state_rows, width), jnp.bfloat16),
        ],
        scratch_shapes=[
            pltpu.VMEM((total, 2 * HD), jnp.float32),
            pltpu.VMEM((state_rows, 2 * HD), jnp.float32),
            pltpu.VMEM((state_rows, 2 * HD), jnp.float32),
        ],
        cost_estimate=pl.CostEstimate(
            flops=10 * total * ENC * width * 2,
            bytes_accessed=12 * total * width + 8 * state_rows * width,
            transcendentals=2 * total * ENC * width // HD,
        ),
        name="cross_backward",
    )(bounds, segments, queries, state_proj, state_proj, out_grads, lse)


def own_columns(weight, pieces):
    c = lax.axis_index("core")
    width = weight.shape[1] // (2 * pieces)
    return [cut(weight, 2 * piece + c, width, 1) for piece in range(pieces)]


def own_row_half(weight):
    return cut(weight, lax.axis_index("core"), weight.shape[0] // 2, 0)


def per_worker(
    hidden_in,
    encoder_states,
    seq_lengths,
    deal,
    gain_self,
    w_self_in,
    w_self_out,
    rel_table,
    gain_cross,
    w_cross_q,
    w_cross_kv,
    w_cross_out,
    gain_ffn,
    w_gate_up,
    w_down,
    grad_out,
):
    y, z, x, c = axis_spots()
    count = lax.axis_size("fsdp")
    blocks = 2 * count
    half_rows = hidden_in.shape[1]
    total_rows = 2 * half_rows
    half_states = encoder_states.shape[1]
    width = hidden_in.shape[2]
    heads_here = HEADS // 2

    order = to_worker(jnp.concatenate([deal[0], seq_lengths[0]]))
    tokens_half = to_worker(hidden_in[0])
    small = jnp.concatenate([gain_self, gain_cross, gain_ffn, rel_table])
    small_all = lax.all_gather(small, "fsdp", axis=0, tiled=False)
    part = gain_self.shape[0]
    gain_one = small_all[:, :part].reshape(-1).astype(jnp.float32)
    gain_two = small_all[:, part : 2 * part].reshape(-1).astype(jnp.float32)
    gain_three = small_all[:, 2 * part : 3 * part].reshape(-1).astype(jnp.float32)
    table_all = small_all[:, 3 * part :].reshape(HEADS, BUCKETS).astype(jnp.float32)
    table = cut(table_all, c, heads_here, 0)

    self_in = gather_blocks(jnp.concatenate(own_columns(w_self_in, 3), axis=1), True, 0)
    states_half = to_worker(encoder_states[0])
    cross_in = gather_blocks(
        jnp.concatenate(own_columns(w_cross_q, 1) + own_columns(w_cross_kv, 2), axis=1), False, 0
    )
    out_block = jnp.concatenate([own_row_half(w_self_out), own_row_half(w_cross_out)], axis=0)
    outs = gather_blocks(out_block, True, 0)
    gate_up = gather_blocks(jnp.concatenate(own_columns(w_gate_up, 2), axis=1), False, 0)
    down = gather_blocks(own_row_half(w_down), True, 1)
    cotangent_half = to_worker(grad_out[0])

    head_width = heads_here * HD
    cross_query = cross_in[:, :head_width]
    cross_kv = cross_in[:, head_width:]
    outs = own_rows_of(outs, count).reshape(count // 2, 2, 2, -1, width)
    self_out = outs[:, :, 0].reshape(-1, width)
    cross_out = outs[:, :, 1].reshape(-1, width)
    down_proj = own_rows_of(down, count)

    tokens = join(c, tokens_half, swap_core(tokens_half), 0)
    states = join(c, states_half, swap_core(states_half), 0)
    cotangent = join(c, cotangent_half, swap_core(cotangent_half), 0)

    dealing = order[:total_rows]
    lengths = order[total_rows:]
    places = jnp.arange(total_rows, dtype=jnp.int32)
    ends = jnp.cumsum(lengths)
    bounds = jnp.concatenate([jnp.zeros((1,), jnp.int32), ends])
    past = (places[:, None] >= ends[None, :]).astype(jnp.int32)
    segments = jnp.sum(past, axis=1, keepdims=True)
    starts = jnp.sum(past * lengths[None, :], axis=1, keepdims=True)
    moves = (places[:, None] == dealing[None, :]).astype(jnp.bfloat16)

    given = dot_nn(moves, tokens)
    normed_one, inverse_one = norm_apply(given, gain_one)
    normed_one = normed_one.astype(jnp.bfloat16)
    projected = dot_nn(normed_one, self_in).astype(jnp.bfloat16)
    attended, self_lse = self_forward(projected, table, starts)
    state_proj = dot_nn(states, cross_kv).astype(jnp.bfloat16)
    partial = dot_nn(attended, self_out).astype(jnp.bfloat16)
    hidden_one = given + (
        partial.astype(jnp.float32) + swap_core(partial).astype(jnp.float32)
    )
    normed_two, inverse_two = norm_apply(hidden_one, gain_two)
    normed_two = normed_two.astype(jnp.bfloat16)
    cross_queries = dot_nn(normed_two, cross_query).astype(jnp.bfloat16)
    crossed, cross_lse = cross_forward(cross_queries, state_proj, bounds, segments)
    partial = dot_nn(crossed, cross_out).astype(jnp.bfloat16)
    hidden_two = hidden_one + (
        partial.astype(jnp.float32) + swap_core(partial).astype(jnp.float32)
    )
    normed_three, inverse_three = norm_apply(hidden_two, gain_three)
    normed_three = normed_three.astype(jnp.bfloat16)
    gate_up_values = dot_nn(normed_three, gate_up)
    units = gate_up.shape[1] // 2
    gate_part = gate_up_values[:, :units]
    up_part = gate_up_values[:, units:]
    gelu_values, gelu_pull = jax.vjp(
        lambda gate_values: jax.nn.gelu(gate_values, approximate=True), gate_part
    )
    activation = (gelu_values * up_part).astype(jnp.bfloat16)
    partial = dot_nn(activation, down_proj).astype(jnp.bfloat16)
    block_half = cut(hidden_two, c, half_rows, 0) + (
        cut(partial, c, half_rows, 0).astype(jnp.float32)
        + swap_core(cut(partial, 1 - c, half_rows, 0)).astype(jnp.float32)
    )
    block_result = to_worker(block_half.astype(jnp.bfloat16))

    grad_down = dot_tn(activation, cotangent).astype(jnp.bfloat16)
    down_low, down_high = reduce_blocks(spread_rows(grad_down, blocks))
    act_grad = dot_nt(cotangent, down_proj)
    gate_grad = gelu_pull(act_grad * up_part)[0].astype(jnp.bfloat16)
    up_grad = (act_grad * gelu_values).astype(jnp.bfloat16)
    gate_up_grad = jnp.concatenate([gate_grad, up_grad], axis=1)
    partial = dot_nt(gate_up_grad, gate_up).astype(jnp.bfloat16)
    normed_three_grad = partial.astype(jnp.float32) + swap_core(partial).astype(jnp.float32)
    grad_gate_up = dot_tn(normed_three, gate_up_grad).astype(jnp.bfloat16)
    gate_up_low, gate_up_high = reduce_blocks(
        grad_gate_up.reshape(blocks, width // blocks, -1)
    )
    hidden_two_part, grad_gain_three = norm_back(
        hidden_two, inverse_three, gain_three, normed_three_grad
    )
    hidden_two_grad = cotangent.astype(jnp.float32) + hidden_two_part
    second_low = hidden_two_grad.astype(jnp.bfloat16)
    crossed_grad = dot_nt(second_low, cross_out).astype(jnp.bfloat16)
    cq_grad, ck_grad, cv_grad = cross_backward(
        cross_queries, state_proj, crossed_grad, cross_lse, bounds, segments
    )
    partial = dot_nt(cq_grad, cross_query).astype(jnp.bfloat16)
    normed_two_grad = partial.astype(jnp.float32) + swap_core(partial).astype(jnp.float32)
    grad_cross_out = dot_tn(crossed, second_low).astype(jnp.bfloat16)
    kv_grad = jnp.concatenate([ck_grad, cv_grad], axis=1)
    grad_cross_q = dot_tn(normed_two, cq_grad).astype(jnp.bfloat16)
    grad_cross_kv = dot_tn(states, kv_grad).astype(jnp.bfloat16)
    block_rows = width // blocks
    cross_out_spread = spread_rows(grad_cross_out, blocks)
    wide = cross_out_spread.shape[2] // 2
    cross_low, cross_high = reduce_blocks(
        jnp.concatenate(
            [
                grad_cross_q.reshape(blocks, block_rows, -1),
                grad_cross_kv.reshape(blocks, block_rows, -1),
                jnp.concatenate(
                    [cross_out_spread[:, :, :wide], cross_out_spread[:, :, wide:]], axis=1
                ),
            ],
            axis=2,
        )
    )
    state_partial = dot_nt(kv_grad, cross_kv).astype(jnp.bfloat16)
    state_half = cut(state_partial, c, half_states, 0).astype(jnp.float32) + swap_core(
        cut(state_partial, 1 - c, half_states, 0)
    ).astype(jnp.float32)
    state_grad = to_worker(state_half.astype(jnp.bfloat16))
    hidden_one_part, grad_gain_two = norm_back(hidden_one, inverse_two, gain_two, normed_two_grad)
    hidden_one_grad = hidden_two_grad + hidden_one_part
    first_low = hidden_one_grad.astype(jnp.bfloat16)
    attended_grad = dot_nt(first_low, self_out).astype(jnp.bfloat16)
    grad_self_out = dot_tn(attended, first_low).astype(jnp.bfloat16)
    self_out_low, self_out_high = reduce_blocks(spread_rows(grad_self_out, blocks))
    sq_grad, sk_grad, sv_grad, table_lines = self_backward(
        projected, attended_grad, self_lse, table, starts
    )
    projected_grad = jnp.concatenate([sq_grad, sk_grad, sv_grad], axis=1)
    grad_self_in = dot_tn(normed_one, projected_grad).astype(jnp.bfloat16)
    self_in_low, self_in_high = reduce_blocks(grad_self_in.reshape(blocks, width // blocks, -1))
    partial = dot_nt(projected_grad, self_in).astype(jnp.bfloat16)
    partial = dot_tn(moves, partial).astype(jnp.bfloat16)
    moves_half = cut(moves, c, half_rows, 1)
    residual_back = dot_tn(moves_half, first_low)
    normed_one_grad = cut(partial, c, half_rows, 0).astype(jnp.float32) + swap_core(
        cut(partial, 1 - c, half_rows, 0)
    ).astype(jnp.float32)
    token_values = tokens_half.astype(jnp.float32)
    token_inverse = lax.rsqrt(
        jnp.mean(token_values * token_values, axis=-1, keepdims=True) + norm_eps
    )
    token_part, grad_gain_one = norm_back(token_values, token_inverse, gain_one, normed_one_grad)
    input_result = to_worker((residual_back + token_part).astype(jnp.bfloat16))

    table_here = jnp.sum(table_lines, axis=-1).reshape(heads_here, BUCKETS)
    grad_table = lax.dynamic_update_slice_in_dim(
        jnp.zeros((HEADS, BUCKETS), jnp.float32), table_here, c * heads_here, 0
    ).reshape(-1)
    small_sum = lax.psum(
        jnp.concatenate([grad_gain_one, 0.5 * grad_gain_two, 0.5 * grad_gain_three, grad_table]),
        AXES,
    )
    spot = y * count + z
    share = width // blocks
    small_parts = [cut(small_sum[at * width : (at + 1) * width], spot, share, 0) for at in range(3)]
    table_part = cut(small_sum[3 * width :], spot, HEADS * BUCKETS // blocks, 0)

    grad_wide = cross_low.shape[1] // 4
    cross_out_low = jnp.concatenate(
        [cross_low[: block_rows // 2, 3 * grad_wide :], cross_low[block_rows // 2 :, 3 * grad_wide :]],
        axis=1,
    )
    cross_out_high = jnp.concatenate(
        [
            cross_high[: block_rows // 2, 3 * grad_wide :],
            cross_high[block_rows // 2 :, 3 * grad_wide :],
        ],
        axis=1,
    )
    return (
        block_result[None],
        input_result[None],
        state_grad[None],
        small_parts[0],
        column_result(self_in_low, self_in_high, 3),
        row_result(self_out_low, self_out_high),
        table_part,
        small_parts[1],
        column_result(cross_low[:, :grad_wide], cross_high[:, :grad_wide], 1),
        column_result(
            cross_low[:, grad_wide : 3 * grad_wide], cross_high[:, grad_wide : 3 * grad_wide], 2
        ),
        row_result(cross_out_low, cross_out_high),
        small_parts[2],
        column_result(gate_up_low, gate_up_high, 2),
        row_result(down_low, down_high),
    )


def split_specs(rep, seq, fsdp):
    groups = P((fsdp,) + rep, seq, None)
    ints = P((fsdp,) + rep, None)
    line = P(fsdp)
    rows = P(fsdp, None)
    line_out = P((seq, fsdp))
    rows_out = P((seq, fsdp), None)
    ins = (groups, groups, ints, ints, line, rows, rows, line, line, rows, rows, rows)
    ins = ins + (line, rows, rows, groups)
    outs = (groups, groups, groups, line_out, rows_out, rows_out, line_out, line_out)
    outs = outs + (rows_out, rows_out, rows_out, line_out, rows_out, rows_out)
    return ins, outs


def solution(mesh):
    sizes = dict(mesh.shape)
    if sizes["seq"] == 2 and sizes["fsdp"] == 4 and sizes["rep"] == 4:
        grid = np.asarray(mesh.devices).reshape(2, 4, 2, 2)
        ins, outs = split_specs(("rx", "core"), "seq", "fsdp")
        return jax.shard_map(
            per_worker, mesh=Mesh(grid, AXES), in_specs=ins, out_specs=outs, check_vma=False
        )
    ins, outs = split_specs(("rep",), "seq", "fsdp")
    return jax.shard_map(per_device, mesh=mesh, in_specs=ins, out_specs=outs, check_vma=False)
```

```python
import functools
import jax
import jax.numpy as jnp
import numpy as np
from jax import lax
from jax.experimental import pallas as pl
from jax.experimental.pallas import tpu as pltpu
from jax.sharding import Mesh
from jax.sharding import PartitionSpec as P

HEADS = 16
HD = 64
BUCKETS = 32
ENC = 384


norm_eps = 1e-06
score_factor = 0.125
masked_score = -1e30
bucket_edges = [int(edge_value) for edge_value in np.ceil(16.0 * 8.0 ** (np.arange(1, 16) / 16.0))]


def bucket_of(distance):
    far_count = jnp.zeros_like(distance)
    for edge_value in bucket_edges:
        far_count = far_count + (distance >= edge_value).astype(jnp.int32)
    return jnp.where(distance < 16, distance, 16 + far_count)


def norm_apply(values, gain):
    inverse = lax.rsqrt(jnp.mean(values * values, axis=-1, keepdims=True) + norm_eps)
    return (values * inverse * gain, inverse)


def norm_back(values, inverse, gain, upstream):
    scaled = values * inverse
    gain_grad = jnp.sum(upstream * scaled, axis=0)
    inner_term = upstream * gain
    value_grad = inverse * (
        inner_term - scaled * jnp.mean(inner_term * scaled, axis=-1, keepdims=True)
    )
    return (value_grad, gain_grad)


def product(left, right):
    return jnp.dot(left, right, preferred_element_type=jnp.float32)


def product_tn(left, right):
    return lax.dot_general(
        left, right, (((0,), (0,)), ((), ())), preferred_element_type=jnp.float32
    )


def product_nt(left, right):
    return lax.dot_general(
        left, right, (((1,), (1,)), ((), ())), preferred_element_type=jnp.float32
    )


def toeplitz_grid(vector, block_len):
    reversed_vec = vector[:, ::-1]
    tiled = jnp.tile(reversed_vec, (1, block_len))
    window = tiled[:, block_len - 1 : block_len - 1 + block_len * (2 * block_len - 2)]
    return window.reshape(vector.shape[0], block_len, 2 * block_len - 2)[:, :, :block_len]


def toeplitz_back(score_grid, block_len):
    rows_here = score_grid.shape[0]
    widened = jnp.pad(score_grid, ((0, 0), (0, 0), (0, block_len - 2)))
    flattened = widened.reshape(rows_here, block_len * (2 * block_len - 2))
    flattened = jnp.pad(flattened, ((0, 0), (block_len - 1, 1)))
    folded = jnp.sum(flattened.reshape(rows_here, block_len, 2 * block_len - 1), axis=1)
    return folded[:, ::-1]


def masked_scores(queries, keys_all, pair_terms, query_size, key_size, query_block, key_block):
    query_part = lax.dynamic_slice_in_dim(queries, query_block * query_size, query_size, 0)
    key_part = lax.dynamic_slice_in_dim(keys_all, key_block * key_size, key_size, 0)
    scores = (
        jnp.einsum("qhd,khd->hqk", query_part, key_part, preferred_element_type=jnp.float32)
        * score_factor
    )
    bias_grid, allowed = pair_terms(query_block, key_block)
    return jnp.where(allowed[None], scores + bias_grid, masked_score)


def attend_forward(queries, keys_all, values_all, pair_terms, key_count, query_size, key_size):
    total_rows, heads_here, head_size = queries.shape

    def stats_step(query_block, lse_all):

        def stats_key_step(key_block, running):
            running_max, running_sum = running
            scores = masked_scores(
                queries, keys_all, pair_terms, query_size, key_size, query_block, key_block
            )
            new_max = jnp.maximum(running_max, jnp.max(scores, axis=-1))
            running_sum = running_sum * jnp.exp(running_max - new_max) + jnp.sum(
                jnp.exp(scores - new_max[:, :, None]), axis=-1
            )
            return (new_max, running_sum)

        initial = (
            jnp.full((heads_here, query_size), masked_score, jnp.float32),
            jnp.zeros((heads_here, query_size), jnp.float32),
        )
        running_max, running_sum = lax.fori_loop(0, key_count(query_block), stats_key_step, initial)
        block_lse = running_max + jnp.log(running_sum)
        return lax.dynamic_update_slice_in_dim(lse_all, block_lse, query_block * query_size, 1)

    lse_all = lax.fori_loop(
        0, total_rows // query_size, stats_step, jnp.zeros((heads_here, total_rows), jnp.float32)
    )

    def value_step(query_block, outputs):
        block_lse = lax.dynamic_slice_in_dim(lse_all, query_block * query_size, query_size, 1)

        def value_key_step(key_block, accum):
            scores = masked_scores(
                queries, keys_all, pair_terms, query_size, key_size, query_block, key_block
            )
            probabilities = jnp.exp(scores - block_lse[:, :, None]).astype(jnp.bfloat16)
            value_part = lax.dynamic_slice_in_dim(values_all, key_block * key_size, key_size, 0)
            return accum + jnp.einsum(
                "hqk,khd->qhd", probabilities, value_part, preferred_element_type=jnp.float32
            )

        accum = lax.fori_loop(
            0,
            key_count(query_block),
            value_key_step,
            jnp.zeros((query_size, heads_here, head_size), jnp.float32),
        )
        return lax.dynamic_update_slice_in_dim(outputs, accum, query_block * query_size, 0)

    outputs = lax.fori_loop(
        0, total_rows // query_size, value_step, jnp.zeros(queries.shape, jnp.float32)
    )
    return (outputs, lse_all)


def attend_backward(
    queries,
    keys_all,
    values_all,
    outputs,
    out_grads,
    lse_all,
    pair_terms,
    key_count,
    query_size,
    key_size,
    bias_back,
    bias_start,
):
    total_rows, heads_here, head_size = queries.shape
    delta_all = jnp.sum(out_grads.astype(jnp.float32) * outputs, axis=-1).T

    def query_step(query_block, outer_carry):
        key_grads, value_grads, query_grads, bias_accum = outer_carry
        row_start = query_block * query_size
        block_lse = lax.dynamic_slice_in_dim(lse_all, row_start, query_size, 1)
        block_delta = lax.dynamic_slice_in_dim(delta_all, row_start, query_size, 1)
        query_part = lax.dynamic_slice_in_dim(queries, row_start, query_size, 0)
        grad_part = lax.dynamic_slice_in_dim(out_grads, row_start, query_size, 0)

        def query_key_step(key_block, inner_carry):
            block_grad, key_grads, value_grads, bias_accum = inner_carry
            scores = masked_scores(
                queries, keys_all, pair_terms, query_size, key_size, query_block, key_block
            )
            probabilities = jnp.exp(scores - block_lse[:, :, None])
            offset = key_block * key_size
            key_part = lax.dynamic_slice_in_dim(keys_all, offset, key_size, 0)
            value_part = lax.dynamic_slice_in_dim(values_all, offset, key_size, 0)
            prob_grad = jnp.einsum(
                "qhd,khd->hqk", grad_part, value_part, preferred_element_type=jnp.float32
            )
            score_grad = (probabilities * (prob_grad - block_delta[:, :, None])).astype(
                jnp.bfloat16
            )
            block_grad = (
                block_grad
                + jnp.einsum(
                    "hqk,khd->qhd", score_grad, key_part, preferred_element_type=jnp.float32
                )
                * score_factor
            )
            key_add = (
                jnp.einsum(
                    "hqk,qhd->khd", score_grad, query_part, preferred_element_type=jnp.float32
                )
                * score_factor
            )
            value_add = jnp.einsum(
                "hqk,qhd->khd",
                probabilities.astype(jnp.bfloat16),
                grad_part,
                preferred_element_type=jnp.float32,
            )
            key_grads = lax.dynamic_update_slice_in_dim(
                key_grads,
                lax.dynamic_slice_in_dim(key_grads, offset, key_size, 0) + key_add,
                offset,
                0,
            )
            value_grads = lax.dynamic_update_slice_in_dim(
                value_grads,
                lax.dynamic_slice_in_dim(value_grads, offset, key_size, 0) + value_add,
                offset,
                0,
            )
            bias_accum = bias_back(bias_accum, query_block, key_block, score_grad)
            return (block_grad, key_grads, value_grads, bias_accum)

        initial = (
            jnp.zeros((query_size, heads_here, head_size), jnp.float32),
            key_grads,
            value_grads,
            bias_accum,
        )
        block_grad, key_grads, value_grads, bias_accum = lax.fori_loop(
            0, key_count(query_block), query_key_step, initial
        )
        query_grads = lax.dynamic_update_slice_in_dim(query_grads, block_grad, row_start, 0)
        return (key_grads, value_grads, query_grads, bias_accum)

    initial_state = (
        jnp.zeros(keys_all.shape, jnp.float32),
        jnp.zeros(values_all.shape, jnp.float32),
        jnp.zeros(queries.shape, jnp.float32),
        bias_start,
    )
    key_grads, value_grads, query_grads, bias_accum = lax.fori_loop(
        0, total_rows // query_size, query_step, initial_state
    )
    return (query_grads, key_grads, value_grads, bias_accum)


def per_device(
    hidden_in,
    encoder_states,
    seq_lengths,
    deal,
    gain_self,
    w_self_in,
    w_self_out,
    rel_table,
    gain_cross,
    w_cross_q,
    w_cross_kv,
    w_cross_out,
    gain_ffn,
    w_gate_up,
    w_down,
    grad_out,
):
    gathered = (
        lax.all_gather(gain_self, "fsdp", axis=0, tiled=True),
        lax.all_gather(w_self_in, "fsdp", axis=0, tiled=True),
        lax.all_gather(w_self_out, "fsdp", axis=0, tiled=True),
        lax.all_gather(rel_table, "fsdp", axis=0, tiled=True),
        lax.all_gather(gain_cross, "fsdp", axis=0, tiled=True),
        lax.all_gather(w_cross_q, "fsdp", axis=0, tiled=True),
        lax.all_gather(w_cross_kv, "fsdp", axis=0, tiled=True),
        lax.all_gather(w_cross_out, "fsdp", axis=0, tiled=True),
        lax.all_gather(gain_ffn, "fsdp", axis=0, tiled=True),
        lax.all_gather(w_gate_up, "fsdp", axis=0, tiled=True),
        lax.all_gather(w_down, "fsdp", axis=0, tiled=True),
    )
    (
        gain_one,
        self_in,
        self_out,
        table_flat,
        gain_two,
        cross_query,
        cross_kv,
        cross_out,
        gain_three,
        gate_up,
        down_proj,
    ) = gathered
    tokens = hidden_in[0]
    states = encoder_states[0]
    lengths = seq_lengths[0]
    dealing = deal[0]
    cotangent = grad_out[0]
    seq_count = lax.axis_size("seq")
    heads_here = HEADS // seq_count
    model_width = tokens.shape[1]
    hidden_units = down_proj.shape[0]
    total_rows = dealing.shape[0]
    state_rows = states.shape[0] * seq_count
    block_size = min(512, total_rows)
    key_size = min(512, state_rows)
    inverse = jnp.argsort(dealing)
    seq_ends = jnp.cumsum(lengths)
    places = jnp.arange(total_rows, dtype=jnp.int32)
    segments = jnp.sum((places[:, None] >= seq_ends[None, :]).astype(jnp.int32), axis=1)
    state_seq = jnp.arange(state_rows, dtype=jnp.int32) // ENC
    head_start = lax.axis_index("seq") * heads_here
    table_here = lax.dynamic_slice_in_dim(
        table_flat.astype(jnp.float32).reshape(HEADS, BUCKETS), head_start, heads_here, 0
    )
    one_hot = (bucket_of(places)[None, :] == jnp.arange(BUCKETS, dtype=jnp.int32)[:, None]).astype(
        jnp.float32
    )
    rel_bias = jnp.dot(table_here, one_hot, precision=lax.Precision.HIGHEST)
    rel_pad = jnp.pad(rel_bias, ((0, 0), (block_size - 1, block_size)))

    def self_pairs(query_block, key_block):
        rows = query_block * block_size + jnp.arange(block_size, dtype=jnp.int32)
        columns = key_block * block_size + jnp.arange(block_size, dtype=jnp.int32)
        row_segments = lax.dynamic_slice_in_dim(segments, query_block * block_size, block_size)
        column_segments = lax.dynamic_slice_in_dim(segments, key_block * block_size, block_size)
        allowed = (rows[:, None] >= columns[None, :]) & (
            row_segments[:, None] == column_segments[None, :]
        )
        vector = lax.dynamic_slice_in_dim(
            rel_pad, (query_block - key_block) * block_size, 2 * block_size - 1, 1
        )
        return (toeplitz_grid(vector, block_size), allowed)

    def self_bias_back(bias_accum, query_block, key_block, score_grad):
        offset = (query_block - key_block) * block_size
        folded = toeplitz_back(score_grad.astype(jnp.float32), block_size)
        updated = lax.dynamic_slice_in_dim(bias_accum, offset, 2 * block_size - 1, 1) + folded
        return lax.dynamic_update_slice_in_dim(bias_accum, updated, offset, 1)

    def cross_pairs(query_block, key_block):
        row_segments = lax.dynamic_slice_in_dim(segments, query_block * block_size, block_size)
        key_segments = lax.dynamic_slice_in_dim(state_seq, key_block * key_size, key_size)
        return (jnp.zeros((), jnp.float32), row_segments[:, None] == key_segments[None, :])

    def cross_bias_back(bias_accum, query_block, key_block, score_grad):
        return bias_accum

    def self_keys(query_block):
        return query_block + 1

    def cross_keys(query_block):
        return state_rows // key_size

    def to_heads(values):
        return values.reshape(values.shape[0], heads_here, HD)

    token_values = tokens.astype(jnp.float32)
    normed_one, inverse_one = norm_apply(token_values, gain_one.astype(jnp.float32))
    normed_one = normed_one.astype(jnp.bfloat16)
    projected = product(normed_one, self_in).astype(jnp.bfloat16)
    query_heads, key_heads, value_heads, token_heads = (
        lax.all_to_all(projected[:, :model_width], "seq", split_axis=1, concat_axis=0, tiled=True),
        lax.all_to_all(
            projected[:, model_width : 2 * model_width],
            "seq",
            split_axis=1,
            concat_axis=0,
            tiled=True,
        ),
        lax.all_to_all(
            projected[:, 2 * model_width :], "seq", split_axis=1, concat_axis=0, tiled=True
        ),
        lax.all_to_all(tokens, "seq", split_axis=1, concat_axis=0, tiled=True),
    )
    query_given = to_heads(jnp.take(query_heads, inverse, axis=0))
    key_given = to_heads(jnp.take(key_heads, inverse, axis=0))
    value_given = to_heads(jnp.take(value_heads, inverse, axis=0))
    token_given = jnp.take(token_heads, inverse, axis=0)
    self_result, self_lse = attend_forward(
        query_given, key_given, value_given, self_pairs, self_keys, block_size, block_size
    )
    self_low = self_result.astype(jnp.bfloat16).reshape(total_rows, heads_here * HD)
    attended_tok, residual_tok = (
        lax.all_to_all(self_low, "seq", split_axis=0, concat_axis=1, tiled=True),
        lax.all_to_all(token_given, "seq", split_axis=0, concat_axis=1, tiled=True),
    )
    hidden_one = residual_tok.astype(jnp.float32) + product(attended_tok, self_out)
    normed_two, inverse_two = norm_apply(hidden_one, gain_two.astype(jnp.float32))
    normed_two = normed_two.astype(jnp.bfloat16)
    cross_query_tok = product(normed_two, cross_query).astype(jnp.bfloat16)
    state_proj = product(states, cross_kv).astype(jnp.bfloat16)
    cross_query_heads, cross_key_heads, cross_value_heads = (
        lax.all_to_all(cross_query_tok, "seq", split_axis=1, concat_axis=0, tiled=True),
        lax.all_to_all(state_proj[:, :model_width], "seq", split_axis=1, concat_axis=0, tiled=True),
        lax.all_to_all(state_proj[:, model_width:], "seq", split_axis=1, concat_axis=0, tiled=True),
    )
    cross_queries = to_heads(cross_query_heads)
    cross_keys_all = to_heads(cross_key_heads)
    cross_values_all = to_heads(cross_value_heads)
    cross_result, cross_lse = attend_forward(
        cross_queries,
        cross_keys_all,
        cross_values_all,
        cross_pairs,
        cross_keys,
        block_size,
        key_size,
    )
    cross_low = cross_result.astype(jnp.bfloat16).reshape(total_rows, heads_here * HD)
    crossed_tok = lax.all_to_all(cross_low, "seq", split_axis=0, concat_axis=1, tiled=True)
    hidden_two = hidden_one + product(crossed_tok, cross_out)
    normed_three, inverse_three = norm_apply(hidden_two, gain_three.astype(jnp.float32))
    normed_three = normed_three.astype(jnp.bfloat16)
    gate_up_values = product(normed_three, gate_up)
    gate_part = gate_up_values[:, :hidden_units]
    up_part = gate_up_values[:, hidden_units:]
    gelu_values, gelu_pull = jax.vjp(
        lambda gate_values: jax.nn.gelu(gate_values, approximate=True), gate_part
    )
    activation = (gelu_values * up_part).astype(jnp.bfloat16)
    block_result = (hidden_two + product(activation, down_proj)).astype(jnp.bfloat16)
    (
        gain_one_b,
        self_in_b,
        self_out_b,
        table_flat_b,
        gain_two_b,
        cross_query_b,
        cross_kv_b,
        cross_out_b,
        gain_three_b,
        gate_up_b,
        down_proj_b,
    ) = gathered
    upstream = cotangent.astype(jnp.float32)
    grad_down = product_tn(activation, cotangent)
    act_grad = product_nt(cotangent, down_proj_b)
    gate_grad = gelu_pull(act_grad * up_part)[0]
    up_grad = act_grad * gelu_values
    gate_up_grad = jnp.concatenate([gate_grad, up_grad], axis=1).astype(jnp.bfloat16)
    grad_gate_up = product_tn(normed_three, gate_up_grad)
    normed_three_grad = product_nt(gate_up_grad, gate_up_b)
    hidden_two_part, grad_gain_three = norm_back(
        hidden_two, inverse_three, gain_three_b.astype(jnp.float32), normed_three_grad
    )
    hidden_two_grad = upstream + hidden_two_part
    second_low = hidden_two_grad.astype(jnp.bfloat16)
    grad_cross_out = product_tn(crossed_tok, second_low)
    crossed_grad = product_nt(second_low, cross_out_b).astype(jnp.bfloat16)
    crossed_grad_heads = lax.all_to_all(
        crossed_grad, "seq", split_axis=1, concat_axis=0, tiled=True
    )
    cq_grad, ck_grad, cv_grad, unused_bias = attend_backward(
        cross_queries,
        cross_keys_all,
        cross_values_all,
        cross_result,
        to_heads(crossed_grad_heads),
        cross_lse,
        cross_pairs,
        cross_keys,
        block_size,
        key_size,
        cross_bias_back,
        jnp.zeros((), jnp.float32),
    )
    cq_tok, ck_tok, cv_tok = (
        lax.all_to_all(
            cq_grad.astype(jnp.bfloat16).reshape(total_rows, heads_here * HD),
            "seq",
            split_axis=0,
            concat_axis=1,
            tiled=True,
        ),
        lax.all_to_all(
            ck_grad.astype(jnp.bfloat16).reshape(state_rows, heads_here * HD),
            "seq",
            split_axis=0,
            concat_axis=1,
            tiled=True,
        ),
        lax.all_to_all(
            cv_grad.astype(jnp.bfloat16).reshape(state_rows, heads_here * HD),
            "seq",
            split_axis=0,
            concat_axis=1,
            tiled=True,
        ),
    )
    grad_cross_query = product_tn(normed_two, cq_tok)
    state_grad_rows = jnp.concatenate([ck_tok, cv_tok], axis=1)
    grad_cross_kv = product_tn(states, state_grad_rows)
    state_grad = product_nt(state_grad_rows, cross_kv_b).astype(jnp.bfloat16)
    normed_two_grad = product_nt(cq_tok, cross_query_b)
    hidden_one_part, grad_gain_two = norm_back(
        hidden_one, inverse_two, gain_two_b.astype(jnp.float32), normed_two_grad
    )
    hidden_one_grad = hidden_two_grad + hidden_one_part
    first_low = hidden_one_grad.astype(jnp.bfloat16)
    grad_self_out = product_tn(attended_tok, first_low)
    attended_grad = product_nt(first_low, self_out_b).astype(jnp.bfloat16)
    attended_grad_heads, residual_grad_heads = (
        lax.all_to_all(attended_grad, "seq", split_axis=1, concat_axis=0, tiled=True),
        lax.all_to_all(first_low, "seq", split_axis=1, concat_axis=0, tiled=True),
    )
    bias_start = jnp.zeros(rel_pad.shape, jnp.float32)
    sq_grad, sk_grad, sv_grad, bias_accum = attend_backward(
        query_given,
        key_given,
        value_given,
        self_result,
        to_heads(attended_grad_heads),
        self_lse,
        self_pairs,
        self_keys,
        block_size,
        block_size,
        self_bias_back,
        bias_start,
    )
    query_dealt = jnp.take(
        sq_grad.astype(jnp.bfloat16).reshape(total_rows, heads_here * HD), dealing, axis=0
    )
    key_dealt = jnp.take(
        sk_grad.astype(jnp.bfloat16).reshape(total_rows, heads_here * HD), dealing, axis=0
    )
    value_dealt = jnp.take(
        sv_grad.astype(jnp.bfloat16).reshape(total_rows, heads_here * HD), dealing, axis=0
    )
    residual_dealt = jnp.take(residual_grad_heads, dealing, axis=0)
    q_tok, k_tok, v_tok, residual_back = (
        lax.all_to_all(query_dealt, "seq", split_axis=0, concat_axis=1, tiled=True),
        lax.all_to_all(key_dealt, "seq", split_axis=0, concat_axis=1, tiled=True),
        lax.all_to_all(value_dealt, "seq", split_axis=0, concat_axis=1, tiled=True),
        lax.all_to_all(residual_dealt, "seq", split_axis=0, concat_axis=1, tiled=True),
    )
    projected_grad = jnp.concatenate([q_tok, k_tok, v_tok], axis=1)
    grad_self_in = product_tn(normed_one, projected_grad)
    normed_one_grad = product_nt(projected_grad, self_in_b)
    token_part, grad_gain_one = norm_back(
        token_values, inverse_one, gain_one_b.astype(jnp.float32), normed_one_grad
    )
    input_result = (residual_back.astype(jnp.float32) + token_part).astype(jnp.bfloat16)
    distance_grad = lax.dynamic_slice_in_dim(bias_accum, block_size - 1, total_rows, 1)
    table_grad_here = jnp.dot(distance_grad, one_hot.T, precision=lax.Precision.HIGHEST)
    grad_table = lax.dynamic_update_slice_in_dim(
        jnp.zeros((HEADS, BUCKETS), jnp.float32), table_grad_here, head_start, 0
    ).reshape(HEADS * BUCKETS)
    summed = (
        lax.psum_scatter(grad_gain_one, ("seq", "fsdp"), scatter_dimension=0, tiled=True),
        lax.psum_scatter(grad_self_in, ("seq", "fsdp"), scatter_dimension=0, tiled=True),
        lax.psum_scatter(grad_self_out, ("seq", "fsdp"), scatter_dimension=0, tiled=True),
        lax.psum_scatter(grad_table, ("seq", "fsdp"), scatter_dimension=0, tiled=True),
        lax.psum_scatter(grad_gain_two, ("seq", "fsdp"), scatter_dimension=0, tiled=True),
        lax.psum_scatter(grad_cross_query, ("seq", "fsdp"), scatter_dimension=0, tiled=True),
        lax.psum_scatter(grad_cross_kv, ("seq", "fsdp"), scatter_dimension=0, tiled=True),
        lax.psum_scatter(grad_cross_out, ("seq", "fsdp"), scatter_dimension=0, tiled=True),
        lax.psum_scatter(grad_gain_three, ("seq", "fsdp"), scatter_dimension=0, tiled=True),
        lax.psum_scatter(grad_gate_up, ("seq", "fsdp"), scatter_dimension=0, tiled=True),
        lax.psum_scatter(grad_down, ("seq", "fsdp"), scatter_dimension=0, tiled=True),
    )
    reduced = (
        lax.psum(summed[0].astype(jnp.bfloat16), "rep").astype(jnp.float32),
        lax.psum(summed[1].astype(jnp.bfloat16), "rep").astype(jnp.float32),
        lax.psum(summed[2].astype(jnp.bfloat16), "rep").astype(jnp.float32),
        lax.psum(summed[3].astype(jnp.bfloat16), "rep").astype(jnp.float32),
        lax.psum(summed[4].astype(jnp.bfloat16), "rep").astype(jnp.float32),
        lax.psum(summed[5].astype(jnp.bfloat16), "rep").astype(jnp.float32),
        lax.psum(summed[6].astype(jnp.bfloat16), "rep").astype(jnp.float32),
        lax.psum(summed[7].astype(jnp.bfloat16), "rep").astype(jnp.float32),
        lax.psum(summed[8].astype(jnp.bfloat16), "rep").astype(jnp.float32),
        lax.psum(summed[9].astype(jnp.bfloat16), "rep").astype(jnp.float32),
        lax.psum(summed[10].astype(jnp.bfloat16), "rep").astype(jnp.float32),
    )
    return (
        block_result[None],
        input_result[None],
        state_grad[None],
        reduced[0],
        reduced[1],
        reduced[2],
        reduced[3],
        reduced[4],
        reduced[5],
        reduced[6],
        reduced[7],
        reduced[8],
        reduced[9],
        reduced[10],
    )


AXES = ("seq", "fsdp", "rx", "core")
TILE = 128


def axis_spots():
    return tuple(lax.axis_index(name) for name in AXES)


def shift_devices(values, mapping):
    sizes = [lax.axis_size(name) for name in AXES]
    pairs = []
    for place in np.ndindex(*sizes):
        target = mapping(*place)
        pairs.append(
            (int(np.ravel_multi_index(place, sizes)), int(np.ravel_multi_index(target, sizes)))
        )
    return lax.ppermute(values, AXES, pairs)


def swap_core(values):
    return shift_devices(values, lambda y, z, x, c: (y, z, x, 1 - c))


def swap_x(values):
    return shift_devices(values, lambda y, z, x, c: (y, z, 1 - x, c))


def swap_y(values):
    return shift_devices(values, lambda y, z, x, c: (1 - y, z, x, c))


def shift_z(values, step):
    count = lax.axis_size("fsdp")
    return shift_devices(values, lambda y, z, x, c: (y, (z + step) % count, x, c))


def to_worker(values):
    return shift_devices(values, lambda y, z, x, c: (c, z, x, y))


def ordered(spot, mine, other):
    return (jnp.where(spot == 0, mine, other), jnp.where(spot == 0, other, mine))


def join(spot, mine, other, axis):
    return jnp.concatenate(ordered(spot, mine, other), axis=axis)


def cut(values, spot, size, axis):
    return lax.dynamic_slice_in_dim(values, spot * size, size, axis)


MESH_ID = pl.DeviceIdType.MESH


def greet(y, z, x, c, count):
    barrier = pltpu.get_barrier_semaphore()
    others = [{"rx": 1 - x}, {"seq": 1 - y}, {"core": 1 - c}]
    others += [{"fsdp": lax.rem(z + step, count)} for step in range(1, count)]
    for other in others:
        pl.semaphore_signal(barrier, inc=1, device_id=other, device_id_type=MESH_ID)
    pl.semaphore_wait(barrier, len(others))


def gather_body(plans, count, *refs):
    total = len(plans)
    ins = refs[:total]
    outs = refs[total : 2 * total - 1]
    small_out = refs[2 * total - 1]
    swapped = refs[2 * total]
    send_sems, recv_sems, local_sems = refs[2 * total + 1 :]
    outs = outs + (small_out,)
    y, z, x, c = axis_spots()
    greet(y, z, x, c, count)
    sources = [None] + [lax.rem(z + count - step, count) for step in range(1, count)]

    def spots(plan):
        return (y, x) if plan["x_first"] else (x, y)

    def region(plan, ref, block, outer, inner):
        rows, columns = plan["shape"]
        if plan["whole"]:
            return ref.at[pl.ds(pl.multiple_of(block * rows, 16), rows), :]
        size = rows if plan["axis"] == 0 else columns
        offset = outer * (size // 2)
        length = size // 2
        if inner is not None:
            offset = offset + inner * (size // 4)
            length = size // 4
        if plan["axis"] == 0:
            start = pl.multiple_of(block * rows + offset, 16)
            return ref.at[pl.ds(start, length), :]
        start = pl.multiple_of(block * rows, 16)
        return ref.at[pl.ds(start, rows), pl.ds(pl.multiple_of(offset, TILE), length)]

    def send(source, target, slot, device):
        return pltpu.make_async_remote_copy(
            src_ref=source,
            dst_ref=target,
            send_sem=send_sems.at[slot],
            recv_sem=recv_sems.at[slot],
            device_id=device,
            device_id_type=MESH_ID,
        )

    first, second, third, local = {}, {}, {}, []
    for at, plan in enumerate(plans):
        outer, inner = spots(plan)
        for step in range(1, count):
            first[at, step] = send(
                region(plan, ins[at], 0, outer, inner),
                region(plan, outs[at], z, outer, inner),
                9 * at + step - 1,
                {"fsdp": lax.rem(z + step, count)},
            )
            first[at, step].start()
        rows = plan["shape"][0]
        own = pltpu.make_async_copy(
            ins[at],
            outs[at].at[pl.ds(pl.multiple_of(z * rows, 16), rows), :],
            local_sems.at[at],
        )
        own.start()
        local.append(own)

    def forward_inner(at):
        plan = plans[at]
        outer, inner = spots(plan)
        for step in range(1, count):
            first[at, step].wait_recv()
            if not plan["whole"]:
                piece = region(plan, outs[at], sources[step], outer, inner)
                device = {"rx": 1 - x} if plan["x_first"] else {"seq": 1 - y}
                second[at, step] = send(piece, piece, 9 * at + 2 + step, device)
                second[at, step].start()

    def forward_outer(at):
        plan = plans[at]
        outer, inner = spots(plan)
        if plan["whole"]:
            return
        for step in range(1, count):
            second[at, step].wait_recv()
            piece = region(plan, outs[at], sources[step], outer, None)
            device = {"seq": 1 - y} if plan["x_first"] else {"rx": 1 - x}
            third[at, step] = send(piece, piece, 9 * at + 5 + step, device)
            third[at, step].start()

    def finish(at):
        plan = plans[at]
        if not plan["whole"]:
            for step in range(1, count):
                third[at, step].wait_recv()
        local[at].wait()
        if plan["swap"]:
            size = (count // 2) * plan["shape"][0]
            start = pl.multiple_of((1 - c) * size, 16)
            last = send(
                outs[at].at[pl.ds(start, size), :], swapped, 9 * total, {"core": 1 - c}
            )
            last.start()
            return [last]
        return []

    tail = []
    for turn in range(total + 2):
        if turn < total:
            forward_inner(turn)
        if 1 <= turn <= total:
            forward_outer(turn - 1)
        if turn >= 2:
            tail += finish(turn - 2)
    for copy in tail:
        copy.wait_recv()
    for copy in list(first.values()) + list(second.values()) + list(third.values()) + tail:
        copy.wait_send()


def gather_all(pieces, plans):
    count = lax.axis_size("fsdp")
    shapes = []
    swap_shape = None
    for piece, plan in zip(pieces, plans):
        rows, columns = piece.shape
        plan["shape"] = (rows, columns)
        shapes.append(jax.ShapeDtypeStruct((count * rows, columns), piece.dtype))
        if plan["swap"]:
            swap_shape = jax.ShapeDtypeStruct((count // 2 * rows, columns), piece.dtype)
    sent = sum(piece.size * 2 for piece in pieces)
    return pl.pallas_call(
        functools.partial(gather_body, plans, count),
        in_specs=[pl.BlockSpec(memory_space=pltpu.VMEM)] * len(pieces),
        out_specs=[pl.BlockSpec(memory_space=pl.ANY)] * (len(pieces) + 1),
        out_shape=shapes + [swap_shape],
        scratch_shapes=[
            pltpu.SemaphoreType.DMA((9 * len(pieces) + 1,)),
            pltpu.SemaphoreType.DMA((9 * len(pieces) + 1,)),
            pltpu.SemaphoreType.DMA((len(pieces),)),
        ],
        compiler_params=pltpu.CompilerParams(collective_id=0, has_side_effects=True),
        cost_estimate=pl.CostEstimate(
            flops=0, bytes_accessed=4 * count * sent, transcendentals=0
        ),
        name="gather_all",
    )(*pieces)


def reduce_body(chunks, count, totals, *refs):
    ins = refs[:totals]
    small = refs[totals]
    outs = refs[totals + 1 : 2 * totals + 1]
    small_out = refs[2 * totals + 1]
    scratch = refs[2 * totals + 2 :]
    buffers = [scratch[3 * at : 3 * at + 3] for at in range(len(chunks))]
    small_sum, small_in, send_sems, recv_sems = scratch[3 * len(chunks) :]
    y, z, x, c = axis_spots()
    greet(y, z, x, c, count)
    sent = []

    def send(source, target, slot, device):
        copy = pltpu.make_async_remote_copy(
            src_ref=source,
            dst_ref=target,
            send_sem=send_sems.at[slot],
            recv_sem=recv_sems.at[slot],
            device_id=device,
            device_id_type=MESH_ID,
        )
        copy.start()
        sent.append(copy)
        return copy

    def lanes(start, size):
        return pl.ds(pl.multiple_of(start, TILE), size)

    def wide(values):
        return values.astype(jnp.float32)

    waits = {}

    def add_rows(rows, left, right, target):
        def one(row, carry):
            target[row] = (wide(left(row)) + wide(right(row))).astype(jnp.bfloat16)
            return carry

        lax.fori_loop(0, rows, one, 0)

    def phase_send(at):
        which, column, width, x_first = chunks[at]
        half = width // 2
        grad = ins[which]
        if x_first:
            source = grad.at[:, :, lanes(column + (1 - x) * half, half)]
            device = {"rx": 1 - x}
        else:
            source = grad.at[pl.ds((1 - y) * count, count), :, column : column + width]
            device = {"seq": 1 - y}
        waits[at, 0] = send(source, buffers[at][0], 7 * at, device)

    def phase_second(at):
        which, column, width, x_first = chunks[at]
        half = width // 2
        grad = ins[which]
        first, second, third = buffers[at]
        waits[at, 0].wait_recv()
        if x_first:
            add_rows(
                2 * count,
                lambda row: grad[row, :, lanes(column + x * half, half)],
                lambda row: first[row],
                first,
            )
            source = first.at[pl.ds((1 - y) * count, count)]
            device = {"seq": 1 - y}
        else:
            add_rows(
                count,
                lambda row: grad[y * count + row, :, column : column + width],
                lambda row: first[row],
                first,
            )
            source = first.at[:, :, lanes((1 - x) * half, half)]
            device = {"rx": 1 - x}
        waits[at, 1] = send(source, second, 7 * at + 1, device)

    def phase_third(at):
        which, column, width, x_first = chunks[at]
        half = width // 2
        first, second, third = buffers[at]
        waits[at, 1].wait_recv()
        if x_first:
            add_rows(
                count, lambda row: first[y * count + row], lambda row: second[row], second
            )
        else:
            add_rows(
                count, lambda row: first[row, :, lanes(x * half, half)], lambda row: second[row], second
            )
        for step in range(1, count):
            target = lax.rem(z + step, count)
            waits[at, 1 + step] = send(
                second.at[target], third.at[step - 1], 7 * at + 1 + step, {"fsdp": target}
            )

    def phase_last(at):
        which, column, width, x_first = chunks[at]
        half = width // 2
        first, second, third = buffers[at]
        for step in range(1, count):
            waits[at, 1 + step].wait_recv()
        value = wide(second[z])
        for step in range(1, count):
            value = value + wide(third[step - 1])
        spot = (c, slice(None), lanes(column + x * half, half))
        outs[which][spot] = value.astype(jnp.bfloat16)
        piece = outs[which].at[spot]
        waits[at, 5] = send(piece, piece, 7 * at + 5, {"rx": 1 - x})

    def phase_core(at):
        which, column, width, x_first = chunks[at]
        waits[at, 5].wait_recv()
        piece = outs[which].at[c, :, column : column + width]
        waits[at, 6] = send(piece, piece, 7 * at + 6, {"core": 1 - c})

    base = 7 * len(chunks)
    small_steps = [{"rx": 1 - x}, {"seq": 1 - y}, {"core": 1 - c}]

    def small_phase(turn):
        if turn == 0:
            small_sum[0] = small[...]
        elif turn <= len(small_steps):
            waits["small", turn - 1].wait_recv()
            small_sum[turn] = small_sum[turn - 1] + small_in[turn - 1]
        if turn < len(small_steps):
            waits["small", turn] = send(
                small_sum.at[turn], small_in.at[turn], base + turn, small_steps[turn]
            )
        elif turn == len(small_steps):
            for step in range(1, count):
                at = len(small_steps) + step - 1
                waits["small", at] = send(
                    small_sum.at[len(small_steps)],
                    small_in.at[at],
                    base + at,
                    {"fsdp": lax.rem(z + step, count)},
                )
        elif turn == len(small_steps) + 1:
            value = small_sum[len(small_steps)]
            for step in range(1, count):
                at = len(small_steps) + step - 1
                waits["small", at].wait_recv()
                value = value + small_in[at]
            small_out[...] = value

    phases = [phase_send, phase_second, phase_third, phase_last, phase_core]
    phase_count = len(phases)
    for at in range(len(chunks)):
        phase_send(at)
    for turn in range(max(len(chunks) + phase_count - 2, len(small_steps) + 2)):
        if turn < len(small_steps) + 2:
            small_phase(turn)
        for number in range(phase_count - 1, 0, -1):
            at = turn - (number - 1)
            if 0 <= at < len(chunks):
                phases[number](at)
    for at in range(len(chunks)):
        waits[at, 6].wait_recv()
    for copy in sent:
        copy.wait_send()


def reduce_all(grads, chunks, small):
    count = lax.axis_size("fsdp")
    scratch = []
    for which, column, width, x_first in chunks:
        rows = grads[which].shape[1]
        first = (2 * count, rows, width // 2) if x_first else (count, rows, width)
        for shape in (first, (count, rows, width // 2), (count - 1, rows, width // 2)):
            scratch.append(pltpu.VMEM(shape, jnp.bfloat16))
    steps = 3 + count - 1
    slots = 7 * len(chunks) + steps
    scratch += [
        pltpu.VMEM((4,) + small.shape, jnp.float32),
        pltpu.VMEM((steps,) + small.shape, jnp.float32),
        pltpu.SemaphoreType.DMA((slots,)),
        pltpu.SemaphoreType.DMA((slots,)),
    ]
    outs = [jax.ShapeDtypeStruct((2,) + grad.shape[1:], grad.dtype) for grad in grads]
    return pl.pallas_call(
        functools.partial(reduce_body, chunks, count, len(grads)),
        in_specs=[pl.BlockSpec(memory_space=pltpu.VMEM)] * (len(grads) + 1),
        out_specs=[pl.BlockSpec(memory_space=pltpu.VMEM)] * (len(grads) + 1),
        out_shape=outs + [jax.ShapeDtypeStruct(small.shape, jnp.float32)],
        scratch_shapes=scratch,
        compiler_params=pltpu.CompilerParams(collective_id=1, has_side_effects=True),
        name="reduce_all",
    )(*grads, small)


def spread_rows(grad, blocks):
    c = lax.axis_index("core")
    half = blocks // 2
    rows = grad.shape[0] // half
    parts = grad.reshape(half, 2, rows // 2, grad.shape[1])
    mine = cut(parts, c, 1, 1)[:, 0]
    other = swap_core(cut(parts, 1 - c, 1, 1)[:, 0])
    return join(c, mine, other, 0)


def column_result(low, high, pieces):
    width = low.shape[1] // pieces
    parts = []
    for piece in range(pieces):
        parts.append(low[:, piece * width : (piece + 1) * width])
        parts.append(high[:, piece * width : (piece + 1) * width])
    return jnp.concatenate(parts, axis=1).astype(jnp.float32)


def row_result(low, high):
    return jnp.concatenate([low, high], axis=0).astype(jnp.float32)


def dot_nn(left, right):
    return lax.dot_general(
        left, right, (((1,), (0,)), ((), ())), preferred_element_type=jnp.float32
    )


def dot_nt(left, right):
    return lax.dot_general(
        left, right, (((1,), (1,)), ((), ())), preferred_element_type=jnp.float32
    )


def dot_tn(left, right):
    return lax.dot_general(
        left, right, (((0,), (0,)), ((), ())), preferred_element_type=jnp.float32
    )


def half_lanes(values, side):
    lanes = lax.broadcasted_iota(jnp.int32, values.shape, 1)
    inside = (lanes >= side * HD) & (lanes < (side + 1) * HD)
    return jnp.where(inside, values, jnp.zeros_like(values))


def pair_lanes(left, right, rows):
    lanes = lax.broadcasted_iota(jnp.int32, (rows, 2 * HD), 1)
    return jnp.where(lanes < HD, left, right)


def fill_bias(bias_ref, table_ref, head, buckets, distance):
    far = table_ref[head, BUCKETS - 1]
    near = jnp.full(buckets.shape, far, jnp.float32)
    for bucket in range(BUCKETS - 1):
        near = jnp.where(buckets == bucket, table_ref[head, bucket], near)
    near = jnp.where(distance < 0, masked_score, near)
    width = bias_ref.shape[1]
    bias_ref[:, : width - 2 * TILE] = jnp.full((TILE, width - 2 * TILE), far, jnp.float32)
    bias_ref[:, width - 2 * TILE :] = near


def near_buckets():
    rows = lax.broadcasted_iota(jnp.int32, (TILE, 2 * TILE), 0)
    columns = lax.broadcasted_iota(jnp.int32, (TILE, 2 * TILE), 1)
    distance = TILE + rows - columns
    return (distance, bucket_of(distance))


def self_scores(query, keys, bias_ref, starts, row):
    size = row + TILE
    width = bias_ref.shape[1]
    scores = dot_nt(query, keys[:size]) + bias_ref[:, width - size :]
    columns = lax.broadcasted_iota(jnp.int32, (TILE, size), 1)
    return jnp.where(columns >= starts, scores, masked_score)


def self_forward_body(table_ref, start_ref, q_ref, k_ref, v_ref, o_ref, lse_ref, bias_ref):
    pair = pl.program_id(0)
    total = q_ref.shape[0]
    distance, buckets = near_buckets()
    keys = k_ref[...]
    outs = {}
    for side in range(2):
        fill_bias(bias_ref, table_ref, 2 * pair + side, buckets, distance)
        query = half_lanes(q_ref[...], side) * jnp.asarray(score_factor, jnp.bfloat16)
        values = half_lanes(v_ref[...], side)
        for row in range(0, total, TILE):
            scores = self_scores(
                query[row : row + TILE], keys, bias_ref, start_ref[row : row + TILE, :], row
            )
            top = jnp.max(scores, axis=-1, keepdims=True)
            weights = jnp.exp(scores - top)
            mass = jnp.sum(weights, axis=-1, keepdims=True)
            low = (weights / mass).astype(jnp.bfloat16)
            outs[side, row] = (dot_nn(low, values[: row + TILE]), top + jnp.log(mass))
    for row in range(0, total, TILE):
        o_ref[row : row + TILE, :] = (outs[0, row][0] + outs[1, row][0]).astype(jnp.bfloat16)
        lse_ref[row : row + TILE, :] = pair_lanes(outs[0, row][1], outs[1, row][1], TILE)


def self_backward_body(
    table_ref,
    start_ref,
    q_ref,
    k_ref,
    v_ref,
    g_ref,
    lse_ref,
    dq_ref,
    dk_ref,
    dv_ref,
    table_grad_ref,
    bias_ref,
    fold_ref,
    dk_sum,
    dv_sum,
):
    pair = pl.program_id(0)
    total = q_ref.shape[0]
    distance, buckets = near_buckets()
    keys = k_ref[...]
    values = v_ref[...]
    width = bias_ref.shape[1]
    dk_sum[...] = jnp.zeros_like(dk_sum)
    dv_sum[...] = jnp.zeros_like(dv_sum)
    dq_parts = {}
    for side in range(2):
        fill_bias(bias_ref, table_ref, 2 * pair + side, buckets, distance)
        fold_ref[...] = jnp.zeros_like(fold_ref)
        query = half_lanes(q_ref[...], side) * jnp.asarray(score_factor, jnp.bfloat16)
        grads = half_lanes(g_ref[...], side)
        side_keys = half_lanes(keys, side)
        for row in range(0, total, TILE):
            size = row + TILE
            rows = slice(row, size)
            scores = self_scores(query[rows], keys, bias_ref, start_ref[rows, :], row)
            weights = jnp.exp(scores - lse_ref[rows, side * HD : side * HD + 1])
            grad_weights = dot_nt(grads[rows], values[:size])
            delta = jnp.sum(weights * grad_weights, axis=-1, keepdims=True)
            grad_scores = weights * (grad_weights - delta)
            fold_ref[:, width - size :] = fold_ref[:, width - size :] + grad_scores
            low = grad_scores.astype(jnp.bfloat16)
            dq_parts[side, row] = dot_nn(low, side_keys[:size]) * score_factor
            dk_sum[:size, :] = dk_sum[:size, :] + dot_tn(low, query[rows])
            dv_sum[:size, :] = dv_sum[:size, :] + dot_tn(weights.astype(jnp.bfloat16), grads[rows])
        near = fold_ref[:, width - 2 * TILE :]
        far = jnp.sum(fold_ref[:, : width - 2 * TILE], axis=0, keepdims=True)
        for bucket in range(BUCKETS):
            line = jnp.sum(jnp.where(buckets == bucket, near, 0.0), axis=0, keepdims=True)
            line = line[:, :TILE] + line[:, TILE:]
            if bucket == BUCKETS - 1:
                for at in range(0, width - 2 * TILE, TILE):
                    line = line + far[:, at : at + TILE]
            table_grad_ref[0, side, bucket : bucket + 1, :] = line
    for row in range(0, total, TILE):
        dq_ref[row : row + TILE, :] = (dq_parts[0, row] + dq_parts[1, row]).astype(jnp.bfloat16)
    dk_ref[...] = dk_sum[...].astype(jnp.bfloat16)
    dv_ref[...] = dv_sum[...].astype(jnp.bfloat16)


def pair_block(rows, offset):
    return pl.BlockSpec((rows, 2 * HD), lambda pair: (0, pair + offset))


def self_forward(projected, table, starts):
    total, width = projected.shape
    heads_here = width // (3 * HD)
    pairs = heads_here // 2
    return pl.pallas_call(
        self_forward_body,
        grid=(pairs,),
        in_specs=[
            pl.BlockSpec(memory_space=pltpu.SMEM),
            pl.BlockSpec((total, 1), lambda pair: (0, 0)),
            pair_block(total, 0),
            pair_block(total, pairs),
            pair_block(total, 2 * pairs),
        ],
        out_specs=[pair_block(total, 0), pair_block(total, 0)],
        out_shape=[
            jax.ShapeDtypeStruct((total, heads_here * HD), jnp.bfloat16),
            jax.ShapeDtypeStruct((total, heads_here * HD), jnp.float32),
        ],
        scratch_shapes=[pltpu.VMEM((TILE, total), jnp.float32)],
        cost_estimate=pl.CostEstimate(
            flops=4 * total * total * HD * heads_here,
            bytes_accessed=12 * total * heads_here * HD,
            transcendentals=total * total * heads_here,
        ),
        name="self_forward",
    )(table, starts, projected, projected, projected)


def self_backward(projected, out_grads, lse, table, starts):
    total, width = projected.shape
    heads_here = width // (3 * HD)
    pairs = heads_here // 2
    one = jax.ShapeDtypeStruct((total, heads_here * HD), jnp.bfloat16)
    return pl.pallas_call(
        self_backward_body,
        grid=(pairs,),
        in_specs=[
            pl.BlockSpec(memory_space=pltpu.SMEM),
            pl.BlockSpec((total, 1), lambda pair: (0, 0)),
            pair_block(total, 0),
            pair_block(total, pairs),
            pair_block(total, 2 * pairs),
            pair_block(total, 0),
            pair_block(total, 0),
        ],
        out_specs=[
            pair_block(total, 0),
            pair_block(total, 0),
            pair_block(total, 0),
            pl.BlockSpec((1, 2, BUCKETS, TILE), lambda pair: (pair, 0, 0, 0)),
        ],
        out_shape=[
            one,
            one,
            one,
            jax.ShapeDtypeStruct((pairs, 2, BUCKETS, TILE), jnp.float32),
        ],
        scratch_shapes=[
            pltpu.VMEM((TILE, total), jnp.float32),
            pltpu.VMEM((TILE, total), jnp.float32),
            pltpu.VMEM((total, 2 * HD), jnp.float32),
            pltpu.VMEM((total, 2 * HD), jnp.float32),
        ],
        cost_estimate=pl.CostEstimate(
            flops=10 * total * total * HD * heads_here,
            bytes_accessed=20 * total * heads_here * HD,
            transcendentals=total * total * heads_here,
        ),
        name="self_backward",
    )(table, starts, projected, projected, projected, out_grads, lse)


def meets(bound_ref, seq, row):
    return (bound_ref[seq] < row + TILE) & (bound_ref[seq + 1] > row)


def cross_forward_body(bound_ref, seg_ref, q_ref, k_ref, v_ref, o_ref, lse_ref):
    total = q_ref.shape[0]
    seq_count = k_ref.shape[0] // ENC
    for row in range(0, total, TILE):
        rows = slice(row, row + TILE)
        for seq in range(seq_count):

            @pl.when(meets(bound_ref, seq, row))
            def one_pair(rows=rows, seq=seq):
                keys = k_ref[seq * ENC : (seq + 1) * ENC, :]
                values = v_ref[seq * ENC : (seq + 1) * ENC, :]
                result = jnp.zeros((TILE, 2 * HD), jnp.float32)
                tops = []
                for side in range(2):
                    query = half_lanes(q_ref[rows, :], side) * jnp.asarray(
                        score_factor, jnp.bfloat16
                    )
                    scores = dot_nt(query, keys)
                    top = jnp.max(scores, axis=-1, keepdims=True)
                    weights = jnp.exp(scores - top)
                    mass = jnp.sum(weights, axis=-1, keepdims=True)
                    low = (weights / mass).astype(jnp.bfloat16)
                    result = result + dot_nn(low, half_lanes(values, side))
                    tops.append(top + jnp.log(mass))
                chosen = seg_ref[rows, :] == seq
                o_ref[rows, :] = jnp.where(chosen, result.astype(jnp.bfloat16), o_ref[rows, :])
                lse_ref[rows, :] = jnp.where(
                    chosen, pair_lanes(tops[0], tops[1], TILE), lse_ref[rows, :]
                )


def cross_backward_body(
    bound_ref,
    seg_ref,
    q_ref,
    k_ref,
    v_ref,
    g_ref,
    lse_ref,
    dq_ref,
    dk_ref,
    dv_ref,
    dq_sum,
    dk_sum,
    dv_sum,
):
    total = q_ref.shape[0]
    seq_count = k_ref.shape[0] // ENC
    dq_sum[...] = jnp.zeros_like(dq_sum)
    dk_sum[...] = jnp.zeros_like(dk_sum)
    dv_sum[...] = jnp.zeros_like(dv_sum)
    for row in range(0, total, TILE):
        rows = slice(row, row + TILE)
        for seq in range(seq_count):

            @pl.when(meets(bound_ref, seq, row))
            def one_pair(rows=rows, seq=seq):
                spot = slice(seq * ENC, (seq + 1) * ENC)
                keys = k_ref[spot, :]
                values = v_ref[spot, :]
                chosen = seg_ref[rows, :] == seq
                for side in range(2):
                    query = half_lanes(q_ref[rows, :], side) * jnp.asarray(
                        score_factor, jnp.bfloat16
                    )
                    grads = half_lanes(g_ref[rows, :], side)
                    scores = dot_nt(query, keys)
                    weights = jnp.exp(scores - lse_ref[rows, side * HD : side * HD + 1])
                    weights = jnp.where(chosen, weights, 0.0)
                    grad_weights = dot_nt(grads, values)
                    delta = jnp.sum(weights * grad_weights, axis=-1, keepdims=True)
                    low = (weights * (grad_weights - delta)).astype(jnp.bfloat16)
                    dq_sum[rows, :] = (
                        dq_sum[rows, :] + dot_nn(low, half_lanes(keys, side)) * score_factor
                    )
                    dk_sum[spot, :] = dk_sum[spot, :] + dot_tn(low, query)
                    dv_sum[spot, :] = dv_sum[spot, :] + dot_tn(weights.astype(jnp.bfloat16), grads)

    dq_ref[...] = dq_sum[...].astype(jnp.bfloat16)
    dk_ref[...] = dk_sum[...].astype(jnp.bfloat16)
    dv_ref[...] = dv_sum[...].astype(jnp.bfloat16)


def cross_forward(queries, state_proj, bounds, segments):
    total, width = queries.shape
    state_rows = state_proj.shape[0]
    pairs = width // (2 * HD)
    return pl.pallas_call(
        cross_forward_body,
        grid=(pairs,),
        in_specs=[
            pl.BlockSpec(memory_space=pltpu.SMEM),
            pl.BlockSpec((total, 1), lambda pair: (0, 0)),
            pair_block(total, 0),
            pair_block(state_rows, 0),
            pair_block(state_rows, pairs),
        ],
        out_specs=[pair_block(total, 0), pair_block(total, 0)],
        out_shape=[
            jax.ShapeDtypeStruct((total, width), jnp.bfloat16),
            jax.ShapeDtypeStruct((total, width), jnp.float32),
        ],
        cost_estimate=pl.CostEstimate(
            flops=4 * total * ENC * width * 2,
            bytes_accessed=8 * total * width + 4 * state_rows * width,
            transcendentals=2 * total * ENC * width // HD,
        ),
        name="cross_forward",
    )(bounds, segments, queries, state_proj, state_proj)


def cross_backward(queries, state_proj, out_grads, lse, bounds, segments):
    total, width = queries.shape
    state_rows = state_proj.shape[0]
    pairs = width // (2 * HD)
    return pl.pallas_call(
        cross_backward_body,
        grid=(pairs,),
        in_specs=[
            pl.BlockSpec(memory_space=pltpu.SMEM),
            pl.BlockSpec((total, 1), lambda pair: (0, 0)),
            pair_block(total, 0),
            pair_block(state_rows, 0),
            pair_block(state_rows, pairs),
            pair_block(total, 0),
            pair_block(total, 0),
        ],
        out_specs=[pair_block(total, 0), pair_block(state_rows, 0), pair_block(state_rows, 0)],
        out_shape=[
            jax.ShapeDtypeStruct((total, width), jnp.bfloat16),
            jax.ShapeDtypeStruct((state_rows, width), jnp.bfloat16),
            jax.ShapeDtypeStruct((state_rows, width), jnp.bfloat16),
        ],
        scratch_shapes=[
            pltpu.VMEM((total, 2 * HD), jnp.float32),
            pltpu.VMEM((state_rows, 2 * HD), jnp.float32),
            pltpu.VMEM((state_rows, 2 * HD), jnp.float32),
        ],
        cost_estimate=pl.CostEstimate(
            flops=10 * total * ENC * width * 2,
            bytes_accessed=12 * total * width + 8 * state_rows * width,
            transcendentals=2 * total * ENC * width // HD,
        ),
        name="cross_backward",
    )(bounds, segments, queries, state_proj, state_proj, out_grads, lse)


def own_columns(weight, pieces):
    c = lax.axis_index("core")
    width = weight.shape[1] // (2 * pieces)
    return [cut(weight, 2 * piece + c, width, 1) for piece in range(pieces)]


def own_row_half(weight):
    return cut(weight, lax.axis_index("core"), weight.shape[0] // 2, 0)


def per_worker(
    hidden_in,
    encoder_states,
    seq_lengths,
    deal,
    gain_self,
    w_self_in,
    w_self_out,
    rel_table,
    gain_cross,
    w_cross_q,
    w_cross_kv,
    w_cross_out,
    gain_ffn,
    w_gate_up,
    w_down,
    grad_out,
):
    y, z, x, c = axis_spots()
    count = lax.axis_size("fsdp")
    blocks = 2 * count
    half_rows = hidden_in.shape[1]
    total_rows = 2 * half_rows
    half_states = encoder_states.shape[1]
    width = hidden_in.shape[2]
    heads_here = HEADS // 2

    order = to_worker(jnp.concatenate([deal[0], seq_lengths[0]]))
    tokens_half = to_worker(hidden_in[0])
    states_half = to_worker(encoder_states[0])
    cotangent_half = to_worker(grad_out[0])
    part = gain_self.shape[0]
    table_part = rel_table.shape[0]
    small = jnp.concatenate([gain_self, gain_cross, gain_ffn, rel_table])
    small = jnp.pad(small, (0, 16 * TILE - small.shape[0])).reshape(16, TILE)
    gate_own, up_own = own_columns(w_gate_up, 2)
    row_block = jnp.concatenate(
        [own_row_half(w_self_out), own_row_half(w_cross_out), own_row_half(w_down)], axis=0
    )
    cross_block = jnp.concatenate(own_columns(w_cross_q, 1) + own_columns(w_cross_kv, 2), axis=1)
    self_block = jnp.concatenate(own_columns(w_self_in, 3), axis=1)

    def plan(x_first, axis=0, whole=False, swap=False):
        return {"x_first": x_first, "axis": axis, "whole": whole, "swap": swap}

    self_in, rows_all, gate_all, up_all, cross_in, small_all, rows_swapped = gather_all(
        [self_block, row_block, gate_own, up_own, cross_block, small],
        [plan(True), plan(False, 1, False, True), plan(True), plan(False), plan(True), plan(True, 0, True)],
    )
    small_all = small_all.reshape(count, -1)
    gain_one = small_all[:, :part].reshape(-1).astype(jnp.float32)
    gain_two = small_all[:, part : 2 * part].reshape(-1).astype(jnp.float32)
    gain_three = small_all[:, 2 * part : 3 * part].reshape(-1).astype(jnp.float32)
    table_all = small_all[:, 3 * part : 3 * part + table_part].reshape(HEADS, BUCKETS)
    table = cut(table_all.astype(jnp.float32), c, heads_here, 0)

    head_width = heads_here * HD
    cross_query = cross_in[:, :head_width]
    cross_kv = cross_in[:, head_width:]
    rows_mine = cut(rows_all, c, rows_swapped.shape[0], 0).reshape(count // 2, -1, width)
    rows_other = rows_swapped.reshape(count // 2, -1, width)
    ends_at = [0]
    for weight in (w_self_out, w_cross_out, w_down):
        ends_at.append(ends_at[-1] + weight.shape[0] // 2)
    self_out, cross_out, down_proj = [
        join(c, rows_mine[:, low:high], rows_other[:, low:high], 1).reshape(-1, width)
        for low, high in zip(ends_at[:-1], ends_at[1:])
    ]

    tokens = join(c, tokens_half, swap_core(tokens_half), 0)
    states = join(c, states_half, swap_core(states_half), 0)
    cotangent = join(c, cotangent_half, swap_core(cotangent_half), 0)

    dealing = order[:total_rows]
    lengths = order[total_rows:]
    places = jnp.arange(total_rows, dtype=jnp.int32)
    ends = jnp.cumsum(lengths)
    bounds = jnp.concatenate([jnp.zeros((1,), jnp.int32), ends])
    past = (places[:, None] >= ends[None, :]).astype(jnp.int32)
    segments = jnp.sum(past, axis=1, keepdims=True)
    starts = jnp.sum(past * lengths[None, :], axis=1, keepdims=True)
    moves = (places[:, None] == dealing[None, :]).astype(jnp.bfloat16)

    given = dot_nn(moves, tokens)
    normed_one, inverse_one = norm_apply(given, gain_one)
    normed_one = normed_one.astype(jnp.bfloat16)
    projected = dot_nn(normed_one, self_in).astype(jnp.bfloat16)
    attended, self_lse = self_forward(projected, table, starts)
    state_proj = dot_nn(states, cross_kv).astype(jnp.bfloat16)
    partial = dot_nn(attended, self_out).astype(jnp.bfloat16)
    hidden_one = given + (
        partial.astype(jnp.float32) + swap_core(partial).astype(jnp.float32)
    )
    normed_two, inverse_two = norm_apply(hidden_one, gain_two)
    normed_two = normed_two.astype(jnp.bfloat16)
    cross_queries = dot_nn(normed_two, cross_query).astype(jnp.bfloat16)
    crossed, cross_lse = cross_forward(cross_queries, state_proj, bounds, segments)
    partial = dot_nn(crossed, cross_out).astype(jnp.bfloat16)
    hidden_two = hidden_one + (
        partial.astype(jnp.float32) + swap_core(partial).astype(jnp.float32)
    )
    normed_three, inverse_three = norm_apply(hidden_two, gain_three)
    normed_three = normed_three.astype(jnp.bfloat16)
    gate_part = dot_nn(normed_three, gate_all)
    up_part = dot_nn(normed_three, up_all)
    gelu_values, gelu_pull = jax.vjp(
        lambda gate_values: jax.nn.gelu(gate_values, approximate=True), gate_part
    )
    activation = (gelu_values * up_part).astype(jnp.bfloat16)
    partial = dot_nn(activation, down_proj).astype(jnp.bfloat16)
    block_half = cut(hidden_two, c, half_rows, 0) + (
        cut(partial, c, half_rows, 0).astype(jnp.float32)
        + swap_core(cut(partial, 1 - c, half_rows, 0)).astype(jnp.float32)
    )
    block_result = to_worker(block_half.astype(jnp.bfloat16))

    grad_down = dot_tn(activation, cotangent).astype(jnp.bfloat16)
    down_spread = spread_rows(grad_down, blocks)
    act_grad = dot_nt(cotangent, down_proj)
    gate_grad = gelu_pull(act_grad * up_part)[0].astype(jnp.bfloat16)
    up_grad = (act_grad * gelu_values).astype(jnp.bfloat16)
    partial = (dot_nt(gate_grad, gate_all) + dot_nt(up_grad, up_all)).astype(jnp.bfloat16)
    normed_three_grad = partial.astype(jnp.float32) + swap_core(partial).astype(jnp.float32)
    block_rows = width // blocks
    grad_gate = dot_tn(normed_three, gate_grad).astype(jnp.bfloat16)
    grad_up = dot_tn(normed_three, up_grad).astype(jnp.bfloat16)
    stacked = []
    for grad in (grad_gate, grad_up):
        grad = grad.reshape(blocks, block_rows, -1)
        stacked += [grad[:, :, at : at + TILE] for at in range(0, grad.shape[2], TILE)]
    stacked += [down_spread[:, :, at : at + TILE] for at in range(0, width, TILE)]
    stacked = jnp.concatenate(stacked, axis=1)
    wide_rows = stacked.shape[1]
    wide_mine = lax.psum_scatter(
        stacked.reshape(-1, TILE), ("seq", "fsdp", "rx"), scatter_dimension=0, tiled=True
    )
    wide_full = join(x, wide_mine, swap_x(wide_mine), 0)
    wide_low, wide_high = ordered(c, wide_full, swap_core(wide_full))
    hidden_two_part, grad_gain_three = norm_back(
        hidden_two, inverse_three, gain_three, normed_three_grad
    )
    hidden_two_grad = cotangent.astype(jnp.float32) + hidden_two_part
    second_low = hidden_two_grad.astype(jnp.bfloat16)
    crossed_grad = dot_nt(second_low, cross_out).astype(jnp.bfloat16)
    cq_grad, ck_grad, cv_grad = cross_backward(
        cross_queries, state_proj, crossed_grad, cross_lse, bounds, segments
    )
    partial = dot_nt(cq_grad, cross_query).astype(jnp.bfloat16)
    normed_two_grad = partial.astype(jnp.float32) + swap_core(partial).astype(jnp.float32)
    grad_cross_out = dot_tn(crossed, second_low).astype(jnp.bfloat16)
    kv_grad = jnp.concatenate([ck_grad, cv_grad], axis=1)
    grad_cross_q = dot_tn(normed_two, cq_grad).astype(jnp.bfloat16)
    grad_cross_kv = dot_tn(states, kv_grad).astype(jnp.bfloat16)
    cross_out_spread = spread_rows(grad_cross_out, blocks)
    state_partial = dot_nt(kv_grad, cross_kv).astype(jnp.bfloat16)
    state_half = cut(state_partial, c, half_states, 0).astype(jnp.float32) + swap_core(
        cut(state_partial, 1 - c, half_states, 0)
    ).astype(jnp.float32)
    state_grad = to_worker(state_half.astype(jnp.bfloat16))
    hidden_one_part, grad_gain_two = norm_back(hidden_one, inverse_two, gain_two, normed_two_grad)
    hidden_one_grad = hidden_two_grad + hidden_one_part
    first_low = hidden_one_grad.astype(jnp.bfloat16)
    attended_grad = dot_nt(first_low, self_out).astype(jnp.bfloat16)
    grad_self_out = dot_tn(attended, first_low).astype(jnp.bfloat16)
    self_out_spread = spread_rows(grad_self_out, blocks)
    sq_grad, sk_grad, sv_grad, table_lines = self_backward(
        projected, attended_grad, self_lse, table, starts
    )
    projected_grad = jnp.concatenate([sq_grad, sk_grad, sv_grad], axis=1)
    grad_self_in = dot_tn(normed_one, projected_grad).astype(jnp.bfloat16)
    partial = dot_nt(projected_grad, self_in).astype(jnp.bfloat16)
    partial = dot_tn(moves, partial).astype(jnp.bfloat16)
    moves_half = cut(moves, c, half_rows, 1)
    residual_back = dot_tn(moves_half, first_low)
    normed_one_grad = cut(partial, c, half_rows, 0).astype(jnp.float32) + swap_core(
        cut(partial, 1 - c, half_rows, 0)
    ).astype(jnp.float32)
    token_values = tokens_half.astype(jnp.float32)
    token_inverse = lax.rsqrt(
        jnp.mean(token_values * token_values, axis=-1, keepdims=True) + norm_eps
    )
    token_part, grad_gain_one = norm_back(token_values, token_inverse, gain_one, normed_one_grad)
    input_result = to_worker((residual_back + token_part).astype(jnp.bfloat16))

    table_here = jnp.sum(table_lines, axis=-1).reshape(heads_here, BUCKETS)
    grad_table = lax.dynamic_update_slice_in_dim(
        jnp.zeros((HEADS, BUCKETS), jnp.float32), table_here, c * heads_here, 0
    ).reshape(-1)
    small_grads = jnp.concatenate(
        [grad_gain_one, 0.5 * grad_gain_two, 0.5 * grad_gain_three, grad_table]
    )
    small_rows = (small_grads.shape[0] + 8 * TILE - 1) // (8 * TILE) * 8
    small_grads = jnp.pad(small_grads, (0, small_rows * TILE - small_grads.shape[0]))
    grads = [
        grad_cross_kv.reshape(blocks, block_rows, -1),
        grad_cross_q.reshape(blocks, block_rows, -1),
        cross_out_spread,
        self_out_spread,
        grad_self_in.reshape(blocks, block_rows, -1),
    ]
    chunks = (
        (0, 0, 512, True),
        (0, 512, 512, False),
        (1, 0, 256, True),
        (1, 256, 256, False),
        (2, 0, 512, True),
        (2, 512, 512, False),
        (3, 0, 512, True),
        (3, 512, 512, False),
        (4, 0, 512, True),
        (4, 512, 512, False),
        (4, 1024, 256, True),
        (4, 1280, 256, False),
    )
    kv_sum, q_sum, cross_out_sum, self_out_sum, self_in_sum, small_sum = reduce_all(
        grads, chunks, small_grads.reshape(small_rows, TILE)
    )
    small_sum = small_sum.reshape(-1)
    spot = y * count + z
    share = width // blocks
    small_parts = [cut(small_sum[at * width : (at + 1) * width], spot, share, 0) for at in range(3)]
    table_part = cut(
        small_sum[3 * width : 3 * width + HEADS * BUCKETS], spot, HEADS * BUCKETS // blocks, 0
    )
    tiles = grad_gate.shape[1] // TILE
    up_at = tiles * block_rows
    down_at = 2 * up_at
    down_rows = down_spread.shape[1]

    def unstack(values, start, rows, pieces):
        return [values[start + at * rows : start + (at + 1) * rows] for at in range(pieces)]

    gate_up_parts = []
    for start in (0, up_at):
        for values in (wide_low, wide_high):
            gate_up_parts += unstack(values, start, block_rows, tiles)
    down_parts = [
        jnp.concatenate(unstack(values, down_at, down_rows, width // TILE), axis=1)
        for values in (wide_low, wide_high)
    ]
    return (
        block_result[None],
        input_result[None],
        state_grad[None],
        small_parts[0],
        column_result(self_in_sum[0], self_in_sum[1], 3),
        row_result(self_out_sum[0], self_out_sum[1]),
        table_part,
        small_parts[1],
        column_result(q_sum[0], q_sum[1], 1),
        column_result(kv_sum[0], kv_sum[1], 2),
        row_result(cross_out_sum[0], cross_out_sum[1]),
        small_parts[2],
        jnp.concatenate(gate_up_parts, axis=1).astype(jnp.float32),
        row_result(down_parts[0], down_parts[1]),
    )


def split_specs(rep, seq, fsdp):
    groups = P((fsdp,) + rep, seq, None)
    ints = P((fsdp,) + rep, None)
    line = P(fsdp)
    rows = P(fsdp, None)
    line_out = P((seq, fsdp))
    rows_out = P((seq, fsdp), None)
    ins = (groups, groups, ints, ints, line, rows, rows, line, line, rows, rows, rows)
    ins = ins + (line, rows, rows, groups)
    outs = (groups, groups, groups, line_out, rows_out, rows_out, line_out, line_out)
    outs = outs + (rows_out, rows_out, rows_out, line_out, rows_out, rows_out)
    return ins, outs


def solution(mesh):
    sizes = dict(mesh.shape)
    if sizes["seq"] == 2 and sizes["fsdp"] == 4 and sizes["rep"] == 4:
        grid = np.asarray(mesh.devices).reshape(2, 4, 2, 2)
        ins, outs = split_specs(("rx", "core"), "seq", "fsdp")
        return jax.shard_map(
            per_worker, mesh=Mesh(grid, AXES), in_specs=ins, out_specs=outs, check_vma=False
        )
    ins, outs = split_specs(("rep",), "seq", "fsdp")
    return jax.shard_map(per_device, mesh=mesh, in_specs=ins, out_specs=outs, check_vma=False)
```
